32 devices in a mesh: dp: 4 (over x, core), tensor: 4 (over z), section: 2 (over y).
Axes of the slice: x: 2, y: 2, z: 4, core: 2. Of those that a mesh axis runs over, the one named last changes fastest.
Arguments:
- patches: bfloat16 [16, 256, 1152], P(('dp', 'section'), 'tensor'), may hold values from -6 to 6
- teacher: int32 [16, 7], P(('dp', 'section')), may hold values from 0 to 255
- proj_w: bfloat16 [1152, 4096], P(None, ('dp', 'tensor', 'section')), may hold values from -0.1875 to 0.1875
- norm_gain: bfloat16 [4096], replicated, may hold values from 0.25 to 1.75
- wq: bfloat16 [4096, 4096], P(('dp', 'section'), 'tensor'), may hold values from -0.09375 to 0.09375
- wk: bfloat16 [4096, 4096], P(('dp', 'section'), 'tensor'), may hold values from -0.09375 to 0.09375
- wv: bfloat16 [4096, 4096], P(('dp', 'section'), 'tensor'), may hold values from -0.09375 to 0.09375
- wo: bfloat16 [4096, 4096], P('tensor', ('dp', 'section')), may hold values from -0.09375 to 0.09375
- start_row: bfloat16 [4096], replicated, may hold values from -6 to 6
- action_table: bfloat16 [256, 4096], replicated, may hold values from -6 to 6
- final_gain: bfloat16 [4096], replicated, may hold values from 0.25 to 1.75
- head_w: bfloat16 [4096, 256], replicated, may hold values from -0.25 to 0.25
Outputs:
- hidden_out: bfloat16 [16, 256, 4096], P(('dp', 'section'), 'tensor')
- loss: float32 [16, 7], P(('dp', 'section'))
The draws below stay inside these ranges and needn't reach their ends.
All inputs are finite; a program needn't handle non-finite values.
Results may differ from the reference program's by a relative error of at most 0.0054.
Values may be sent and summed in bfloat16 or wider, within the bound.
A program may use at most 128 MiB of HBM per device.

```python
import math
import jax
import jax.numpy as jnp
from jax import lax

D = 4096
HEADS = 32
HD = 128
V = 1152
P_SIZE = 256
BINS = 256
ADIM = 7
SLOTS = 8
FRAMES = 16


def touch_ends(values, rng, low, largest):
    place = [jax.random.randint(jax.random.fold_in(rng, axis), (), 0, length) for axis, length in enumerate(values.shape)]
    main_axis = values.shape.index(max(values.shape))
    beside = place[:main_axis] + [(place[main_axis] + 1) % values.shape[main_axis]] + place[main_axis + 1:]
    return values.at[tuple(place)].set(low).at[tuple(beside)].set(largest)


def shard_levels(rng, shape, pieces, smallest, largest):
    def one(axis_at, blocks):
        heights = jax.random.uniform(jax.random.fold_in(jax.random.fold_in(rng, 6), axis_at), (blocks,), jnp.float32, smallest / len(pieces), largest / len(pieces))
        return jnp.repeat(jnp.exp(heights), shape[axis_at] // blocks).reshape((-1,) + (1,) * (len(shape) - axis_at - 1))

    loudness = one(*pieces[0])
    for cut in pieces[1:]:
        loudness = loudness * one(*cut)
    return loudness


def scatter_about(own_key, shape, deviation, reach, cuts=(), kind=jnp.bfloat16):
    array = jax.random.normal(own_key, shape, jnp.float32) * deviation
    if len(cuts) > 0:
        array = shard_levels(own_key, shape, cuts, -0.22, 0.18) * array
    return jnp.clip(array, min=-reach, max=reach).astype(kind)


def setup_inputs(seed: int = 0) -> dict:
    splits = jax.random.split(jax.random.key(seed), 13)
    return {
        "patches": scatter_about(splits[0], (FRAMES, P_SIZE, V), 1.0, 6.0, ((0, 8), (1, 4))),
        "teacher": touch_ends(jax.random.randint(splits[1], (FRAMES, ADIM), 0, BINS), jax.random.fold_in(splits[1], 1), 0, BINS - 1).astype(jnp.int32),
        "proj_w": scatter_about(splits[2], (V, D), V ** -0.5, 0.1875, ((1, 32),)),
        "norm_gain": jnp.clip(1.0 + 0.15 * jax.random.normal(splits[3], (D,), jnp.float32), 0.25, 1.75).astype(jnp.bfloat16),
        "wq": scatter_about(splits[4], (D, D), D ** -0.5, 0.09375, ((0, 8), (1, 4))),
        "wk": scatter_about(splits[5], (D, D), D ** -0.5, 0.09375, ((0, 8), (1, 4))),
        "wv": scatter_about(splits[6], (D, D), D ** -0.5, 0.09375, ((0, 8), (1, 4))),
        "wo": scatter_about(splits[7], (D, D), D ** -0.5, 0.09375, ((0, 4), (1, 8))),
        "start_row": scatter_about(splits[8], (D,), 1.0, 6.0),
        "action_table": scatter_about(splits[9], (BINS, D), 1.0, 6.0),
        "final_gain": jnp.clip(1.0 + 0.15 * jax.random.normal(splits[10], (D,), jnp.float32), 0.25, 1.75).astype(jnp.bfloat16),
        "head_w": scatter_about(splits[11], (D, BINS), (D // 9) ** -0.5, 0.25),
    }


eps = 1e-05

def normalize(rows, gain):
    rows = rows.astype(jnp.float32)
    factor = lax.rsqrt(lax.optimization_barrier(jnp.mean(rows * rows, axis=-1, keepdims=True)) + eps)
    return rows * factor * gain.astype(jnp.float32)

def action_rows(teacher, start_row, action_table):
    frames = teacher.shape[0]
    onehot = (teacher[..., None] == jnp.arange(BINS, dtype=jnp.int32)).astype(jnp.bfloat16)
    looked = jnp.dot(onehot.reshape(-1, BINS), action_table, preferred_element_type=jnp.float32)
    looked = looked.astype(jnp.bfloat16).reshape(frames, ADIM, D)
    start = jnp.broadcast_to(start_row.reshape(1, 1, D), (frames, 1, D))
    return jnp.concatenate([start, looked], axis=1)

def reference(patches, teacher, proj_w, norm_gain, wq, wk, wv, wo, start_row, action_table, final_gain, head_w):
    frames = patches.shape[0]
    length = P_SIZE + SLOTS
    embedded = jnp.dot(patches.reshape(-1, V), proj_w, preferred_element_type=jnp.float32)
    embedded = embedded.astype(jnp.bfloat16).reshape(frames, P_SIZE, D)
    actions = action_rows(teacher, start_row, action_table)
    stream = jnp.concatenate([embedded, actions], axis=1)
    normed = normalize(stream, norm_gain).astype(jnp.bfloat16).reshape(-1, D)
    queries = jnp.dot(normed, wq, preferred_element_type=jnp.float32).astype(jnp.bfloat16).reshape(frames, length, HEADS, HD)
    keys_all = jnp.dot(normed, wk, preferred_element_type=jnp.float32).astype(jnp.bfloat16).reshape(frames, length, HEADS, HD)
    values_all = jnp.dot(normed, wv, preferred_element_type=jnp.float32).astype(jnp.bfloat16).reshape(frames, length, HEADS, HD)
    positions = jnp.arange(length, dtype=jnp.int32)
    causal = positions[:, None] >= positions[None, :]
    inv_root = 1.0 / math.sqrt(HD)

    def one_frame(items):
        query_f, key_f, value_f = items
        scores = jnp.einsum('qhd,khd->hqk', query_f.astype(jnp.float32), key_f.astype(jnp.float32)) * inv_root
        scores = jnp.where(causal[None], scores, -1e+30)
        weights = jax.nn.softmax(scores, axis=-1).astype(jnp.bfloat16)
        result = jnp.einsum('hqk,khd->qhd', weights.astype(jnp.float32), value_f.astype(jnp.float32))
        return result.astype(jnp.bfloat16)
    mixed = lax.map(one_frame, (queries, keys_all, values_all)).reshape(-1, D)
    update = jnp.dot(mixed, wo, preferred_element_type=jnp.float32).reshape(frames, length, D)
    hidden_out = (embedded.astype(jnp.float32) + update[:, :P_SIZE]).astype(jnp.bfloat16)
    acted = actions[:, :ADIM].astype(jnp.float32) + update[:, P_SIZE:P_SIZE + ADIM]
    final = normalize(acted, final_gain).astype(jnp.bfloat16).reshape(-1, D)
    logits = jnp.dot(final, head_w, preferred_element_type=jnp.float32).reshape(frames, ADIM, BINS)
    chosen = (teacher[..., None] == jnp.arange(BINS, dtype=jnp.int32)).astype(jnp.float32)
    picked = lax.optimization_barrier(jnp.sum(logits * chosen, axis=-1))
    loss = jax.nn.logsumexp(logits, axis=-1) - picked
    return (hidden_out, loss)
```

```python
import functools
import math

import jax
import jax.numpy as jnp
from jax import lax
from jax.experimental import pallas as pl
from jax.experimental.pallas import tpu as pltpu
from jax.sharding import PartitionSpec as P

D = 4096
HD = 128
V = 1152
P_SIZE = 256
BINS = 256
ADIM = 7
SLOTS = 8


eps = 1e-05


def normalize(rows, gain):
    rows = rows.astype(jnp.float32)
    factor = lax.rsqrt(jnp.mean(rows * rows, axis=-1, keepdims=True) + eps)
    return rows * factor * gain.astype(jnp.float32)


def action_rows(teacher, start_row, action_table):
    frames = teacher.shape[0]
    onehot = (teacher[..., None] == jnp.arange(BINS, dtype=jnp.int32)).astype(jnp.bfloat16)
    looked = jnp.dot(onehot.reshape(-1, BINS), action_table, preferred_element_type=jnp.float32)
    looked = looked.astype(jnp.bfloat16).reshape(frames, ADIM, D)
    start = jnp.broadcast_to(start_row.reshape(1, 1, D), (frames, 1, D))
    return jnp.concatenate([start, looked], axis=1)


def line_gather(own, axis):
    n = lax.axis_size(axis)
    here = lax.axis_index(axis)
    right = left = own
    from_left, from_right = [], []
    for r in range(n - 1):
        right = lax.ppermute(right, axis, [(t, t + 1) for t in range(r, n - 1)])
        left = lax.ppermute(left, axis, [(t, t - 1) for t in range(1, n - r)])
        from_left.append(right)
        from_right.append(left)
    blocks = jnp.zeros((n,) + own.shape, own.dtype)
    blocks = lax.dynamic_update_index_in_dim(blocks, own, here, 0)
    for r in range(n - 1):
        block = jnp.where(here > r, from_left[r], from_right[n - 2 - r])
        blocks = lax.dynamic_update_index_in_dim(blocks, block, lax.rem(here - 1 - r + n, n), 0)
    return blocks


def line_reduce_scatter(parts, axis):
    n = lax.axis_size(axis)
    here = lax.axis_index(axis)

    def part(c):
        return lax.dynamic_index_in_dim(parts, jnp.clip(c, 0, n - 1), 0, keepdims=False)

    right = left = None
    for r in range(n - 1):
        steps = range(min(r, n - 2) + 1)
        to_right = part(n - 1 - r + here)
        to_left = part(r - (n - 1) + here)
        if right is not None:
            to_right = to_right + right.astype(jnp.float32)
            to_left = to_left + left.astype(jnp.float32)
        right = lax.ppermute(to_right.astype(jnp.bfloat16), axis, [(t, t + 1) for t in steps])
        left = lax.ppermute(
            to_left.astype(jnp.bfloat16), axis, [(n - 1 - t, n - 2 - t) for t in steps]
        )
    total = part(here)
    if right is not None:
        total = total + right.astype(jnp.float32) + left.astype(jnp.float32)
    return total


def plane_columns(own):
    rows, columns = own.shape
    blocks = line_gather(line_gather(own, "section").reshape(-1, columns), "dp")
    blocks = blocks.reshape(-1, rows, columns)
    return jnp.concatenate([blocks[i] for i in range(blocks.shape[0])], axis=1)


RELAYS = 2


def on_device(
    patches, teacher, proj_w, norm_gain, wq, wk, wv, wo, start_row, action_table, final_gain, head_w
):
    frames = patches.shape[0]
    local_patches = patches.shape[1]
    length = P_SIZE + SLOTS
    plane = ("dp", "section")
    n_dp, n_t = lax.axis_size("dp"), lax.axis_size("tensor")
    here = lax.axis_index("tensor")
    proj_part = plane_columns(proj_w)
    all_patches = line_gather(patches.reshape(-1, V), "tensor")
    all_patches = all_patches.reshape(n_t, frames, local_patches, V).transpose(1, 0, 2, 3)
    embedded_part = jnp.dot(
        all_patches.reshape(-1, V), proj_part, preferred_element_type=jnp.float32
    ).astype(jnp.bfloat16)
    blocks = line_gather(embedded_part, "tensor")
    width = embedded_part.shape[1] // n_dp
    embedded_all = jnp.concatenate(
        [blocks[t, :, d * width : (d + 1) * width] for d in range(n_dp) for t in range(n_t)], axis=1
    ).reshape(frames, P_SIZE, D)
    embedded_own = lax.dynamic_slice_in_dim(embedded_all, here * local_patches, local_patches, 1)
    actions = action_rows(teacher, start_row, action_table)
    stream = jnp.concatenate([embedded_all, actions], axis=1)
    normed = normalize(stream, norm_gain).astype(jnp.bfloat16).reshape(-1, D)
    full_out = plane_columns(wo)
    local_width = wq.shape[1]
    projected = tuple(
        jnp.dot(
            normed,
            lax.all_gather(weight, plane, axis=0, tiled=True),
            preferred_element_type=jnp.float32,
        )
        for weight in (wq, wk, wv)
    )
    heads_local = local_width // HD
    queries, keys_all, values_all = [
        part.astype(jnp.bfloat16).reshape(frames, length, heads_local, HD) for part in projected
    ]
    inv_root = 1.0 / math.sqrt(HD)
    scores = (
        jnp.einsum("fqhd,fkhd->fhqk", queries, keys_all, preferred_element_type=jnp.float32)
        * inv_root
    )
    positions = jnp.arange(length, dtype=jnp.int32)
    causal = positions[:, None] >= positions[None, :]
    scores = jnp.where(causal[None, None], scores, -1e30)
    weights = jax.nn.softmax(scores, axis=-1).astype(jnp.bfloat16)
    mixed = jnp.einsum("fhqk,fkhd->fqhd", weights, values_all, preferred_element_type=jnp.float32)
    mixed = mixed.astype(jnp.bfloat16).reshape(frames, length, local_width)
    patch_rows = mixed[:, :P_SIZE].reshape(frames, n_t, local_patches, local_width)
    patch_rows = patch_rows.transpose(1, 0, 2, 3).reshape(n_t, -1, local_width)
    slot_rows = mixed[:, P_SIZE:].reshape(-1, local_width)
    slot_part = jnp.dot(slot_rows, full_out, preferred_element_type=jnp.float32)
    slot_parts = line_gather(slot_part.astype(jnp.bfloat16), "tensor")
    slot_update = jnp.sum(slot_parts.astype(jnp.float32), axis=0)
    chunk = D // RELAYS
    updates = []
    for j in range(RELAYS):
        parts = jnp.einsum(
            "nrw,wc->nrc",
            patch_rows,
            full_out[:, j * chunk : (j + 1) * chunk],
            preferred_element_type=jnp.float32,
        )
        updates.append(line_reduce_scatter(parts, "tensor"))
    update = jnp.concatenate(updates, axis=1).reshape(frames, local_patches, D)
    hidden_out = (embedded_own.astype(jnp.float32) + update).astype(jnp.bfloat16)
    acted = (actions.astype(jnp.float32) + slot_update.reshape(frames, SLOTS, D))[:, :ADIM]
    final = normalize(acted, final_gain).astype(jnp.bfloat16).reshape(-1, D)
    logits = jnp.dot(final, head_w, preferred_element_type=jnp.float32).reshape(frames, ADIM, BINS)
    chosen = (teacher[..., None] == jnp.arange(BINS, dtype=jnp.int32)).astype(jnp.float32)
    picked = jnp.sum(logits * chosen, axis=-1)
    loss = jax.nn.logsumexp(logits, axis=-1) - picked
    return (hidden_out, loss)


MESH = pl.DeviceIdType.MESH
ROWS = 128
F32 = jnp.float32
BF16 = jnp.bfloat16


def aligned(value, to=128):
    return pl.multiple_of(value, to)


def fused(
    sizes,
    gain_ref, start_ref, final_gain_ref, lookup_ref, chosen_ref,
    patches_hbm, proj_hbm, wq_hbm, wk_hbm, wv_hbm, wo_hbm, table_hbm, head_hbm,
    out_ref, loss_ref,
    w_ref, wo_ref, quarter, pair, patch, table, head,
    send_c, recv_c, send_1, recv_1, send_2, recv_2, own_c, own_1, own_2, merged,
    total, qkv, mixed, emb, squares, squares_in, factor, factor_in,
    act, nact, nact_all, apart, apart_in, qkv_act, mixed_act, aup, aup_in, asq, asq_in, alog, alog_in,
    right_out, left_out, right_in, left_in, part,
    local_sem, py_s, py_r, px_s, px_r, pd_s, pd_r, pc_s, pc_r, zr_s, zl_s, z_r,
    pz_s, pz_r, na_s, na_r, ap_s, ap_r, c_s, c_r, s1_s, s1_r, s2_s, s2_r, g2_s, g2_r, g1_s, g1_r, gc_s, gc_r,
    sq_s, sq_r, fa_s, fa_r, wo_s, wo_r, rr_s, rr_r, rl_s, rl_r, au_s, au_r, aq_s, aq_r, al_s, al_r,
):
    n_t, frames, local = sizes
    dp, z, y = lax.axis_index("dp"), lax.axis_index("tensor"), lax.axis_index("section")
    c, x = dp % 2, dp // 2
    me = dp * 2 + y
    dp_x, dp_c, y_n = dp + 2 - 4 * x, dp + 1 - 2 * c, 1 - y
    dev_1 = (dp + (1 - c) * (2 - 4 * x), z, y + c * (1 - 2 * y))
    dev_2 = (dp + c * (2 - 4 * x), z, y + (1 - c) * (1 - 2 * y))
    dev_c, dev_x, dev_y = (dp_c, z, y), (dp_x, z, y), (dp, z, y_n)
    b1, b2 = (1 - c) * x + c * y, (1 - c) * y + c * x
    rows = frames * local
    depth, width = wq_hbm.shape
    cols = proj_hbm.shape[1]
    vision = proj_hbm.shape[0]
    chunks = vision // ROWS
    wide = 3 * width
    half, fourth, eighth = wide // 2, wide // 4, wide // 8
    pairs = n_t // 2
    duo = 2 * cols
    heads = width // HD

    def remote(src, dst, send, recv, device):
        return pltpu.make_async_remote_copy(
            src_ref=src, dst_ref=dst, send_sem=send, recv_sem=recv, device_id=device, device_id_type=MESH
        )

    def plane_peer(m):
        g = (me + m) % 8
        return g, (g // 2, z, g % 2)

    own_col = aligned(y * cols, cols)
    loads = [
        pltpu.make_async_copy(proj_hbm, quarter.at[dp, :, pl.ds(own_col, cols)], local_sem.at[0]),
        pltpu.make_async_copy(patches_hbm, patch.at[z], local_sem.at[1]),
        pltpu.make_async_copy(table_hbm, table, local_sem.at[2]),
        pltpu.make_async_copy(wq_hbm, w_ref.at[:, pl.ds(0, width)], local_sem.at[3]),
        pltpu.make_async_copy(wk_hbm, w_ref.at[:, pl.ds(width, width)], local_sem.at[4]),
        pltpu.make_async_copy(wv_hbm, w_ref.at[:, pl.ds(2 * width, width)], local_sem.at[5]),
        pltpu.make_async_copy(wo_hbm, wo_ref.at[me], local_sem.at[6]),
    ]
    for load in loads:
        load.start()

    barrier = pltpu.get_barrier_semaphore()
    for m in range(1, 8):
        pl.semaphore_signal(barrier, inc=1, device_id=plane_peer(m)[1], device_id_type=MESH)
    for k in range(1, n_t):
        pl.semaphore_signal(barrier, inc=1, device_id=(dp, (z + k) % n_t, y), device_id_type=MESH)
    pl.semaphore_wait(barrier, 7 + n_t - 1)

    def rows_of(i):
        return pl.ds(aligned(i * ROWS, ROWS), ROWS)

    def proj_y(i):
        block = quarter.at[dp, rows_of(i), pl.ds(own_col, cols)]
        return remote(block, block, py_s.at[i], py_r.at[i], dev_y)

    def proj_x():
        block = quarter.at[dp, :, pl.ds(own_col, cols)]
        return remote(block, block, px_s, px_r, dev_x)

    def proj_diag():
        at = dp * (1 - c) + dp_x * c
        col = aligned(((1 - c) * (1 - y) + c * y) * cols, cols)
        block = quarter.at[at, :, pl.ds(col, cols)]
        return remote(block, block, pd_s, pd_r, dev_1)

    def proj_core(k):
        block = quarter.at[(dp, dp_x)[k]]
        return remote(block, block, pc_s.at[k], pc_r.at[k], dev_c)

    def patch_send(k, g):
        third = vision // 3
        block = patch.at[z, :, pl.ds(g * third, third)]
        return remote(block, block, pz_s.at[k - 1, g], pz_r.at[k - 1, g], (dp, (z + k) % n_t, y))

    def act_send(m):
        g, device = plane_peer(m)
        col = aligned(g * depth, depth)
        return remote(nact.at[:, pl.ds(col, depth)], nact_all.at[me], na_s.at[m - 1], na_r.at[m - 1], device)

    def apart_send(m):
        g, device = plane_peer(m)
        return remote(apart.at[g], apart_in.at[me], ap_s.at[m - 1], ap_r.at[m - 1], device)

    loads[0].wait()
    for i in range(chunks):
        proj_y(i).start()
    proj_x().start()

    loads[2].wait()
    looked = jnp.dot(lookup_ref[...], table[...], preferred_element_type=F32)
    slot = lax.broadcasted_iota(jnp.int32, looked.shape, 0) % SLOTS
    act[...] = jnp.where(slot == 0, start_ref[...].astype(F32), looked)
    rows_f = act[...]
    scale = lax.rsqrt(jnp.mean(rows_f * rows_f, axis=-1, keepdims=True) + eps)
    nact[...] = (rows_f * scale * gain_ref[...].astype(F32)).astype(BF16)
    nact_all[me] = nact[:, pl.ds(aligned(me * depth, depth), depth)]
    for m in range(1, 8):
        act_send(m).start()
    loads[1].wait()
    for k in (3, 4, 5):
        loads[k].wait()
    for m in range(1, 8):
        act_send(m).wait_recv()
    slots = nact.shape[0]
    stacked = nact_all[...].reshape(8 * slots, depth)
    tile = 512

    def act_tile(j, carry):
        at = pl.ds(aligned(j * tile, tile), tile)
        value = jnp.dot(stacked, w_ref[:, at], preferred_element_type=F32).astype(BF16)
        apart[:, :, at] = value.reshape(8, slots, tile)
        return carry

    lax.fori_loop(0, wide // tile, act_tile, 0)
    apart_in[me] = apart[me]
    for m in range(1, 8):
        apart_send(m).start()

    gain_own = gain_ref[:, pl.ds(aligned(me * depth, depth), depth)].astype(F32)

    def z_right(p, i, own):
        src = quarter.at[dp, rows_of(i)] if own else pair.at[p, rows_of(i)]
        return remote(src, pair.at[p, rows_of(i)], zr_s.at[p, i], z_r.at[p, i], (dp, lax.rem(z + 1, n_t), y))

    def z_left(p, i, own):
        src = quarter.at[dp, rows_of(i)] if own else pair.at[p, rows_of(i)]
        return remote(src, pair.at[p, rows_of(i)], zl_s.at[p, i], z_r.at[p, i], (dp, lax.rem(z + n_t - 1, n_t), y))

    def spread(i):
        proj_y(i).wait_recv()
        for p in range(pairs):
            home = pairs * y + p

            @pl.when(z == home)
            def _():
                @pl.when(z < n_t - 1)
                def _():
                    z_right(p, i, True).start()

                @pl.when(z > 0)
                def _():
                    z_left(p, i, True).start()

                pair[p, rows_of(i)] = quarter[dp, rows_of(i)]

            @pl.when(z > home)
            def _():
                z_right(p, i, False).wait_recv()

                @pl.when(z < n_t - 1)
                def _():
                    z_right(p, i, False).start()

            @pl.when(z < home)
            def _():
                z_left(p, i, False).wait_recv()

                @pl.when(z > 0)
                def _():
                    z_left(p, i, False).start()

    def spread_done(i):
        for p in range(pairs):
            home = pairs * y + p

            @pl.when((z >= home) & (z < n_t - 1))
            def _():
                z_right(p, i, False).wait_send()

            @pl.when((z <= home) & (z > 0))
            def _():
                z_left(p, i, False).wait_send()

    off_c = c * half
    off_1 = off_c + b1 * fourth
    off_2 = off_1 + b2 * eighth

    def at_c(i):
        return remote(send_c.at[i % 2], recv_c.at[i], c_s.at[i], c_r.at[i], dev_c)

    def at_1(i):
        return remote(send_1.at[i % 2], recv_1.at[i], s1_s.at[i], s1_r.at[i], dev_1)

    def at_2(i):
        return remote(send_2.at[i % 2], recv_2.at[i], s2_s.at[i], s2_r.at[i], dev_2)

    def back_2(i):
        block = merged.at[rows_of(i), pl.ds(aligned(off_2), eighth)]
        return remote(block, block, g2_s.at[i], g2_r.at[i], dev_2)

    def back_1(i):
        block = merged.at[rows_of(i), pl.ds(aligned(off_1), fourth)]
        return remote(block, block, g1_s.at[i], g1_r.at[i], dev_1)

    def back_c(i):
        block = merged.at[rows_of(i), pl.ds(aligned(off_c), half)]
        return remote(block, block, gc_s.at[i], gc_r.at[i], dev_c)

    def stage_c(i):
        @pl.when(i >= 2)
        def _():
            at_c(i - 2).wait_send()

        block = jnp.concatenate([pair[p, rows_of(i)] for p in range(pairs)], axis=1)
        block = (block.astype(F32) * gain_own).astype(BF16)

        def away(j, carry):
            at = pl.ds(aligned((1 - c) * half + j * tile), tile)
            value = jnp.dot(block, w_ref[:, at], preferred_element_type=F32)
            send_c[i % 2, :, pl.ds(aligned(j * tile, tile), tile)] = value.astype(BF16)
            return carry

        lax.fori_loop(0, half // tile, away, 0)
        at_c(i).start()

        def kept(j, carry):
            at = pl.ds(aligned(c * half + j * tile), tile)
            own_c[:, pl.ds(aligned(j * tile, tile), tile)] = jnp.dot(block, w_ref[:, at], preferred_element_type=F32)
            return carry

        lax.fori_loop(0, half // tile, kept, 0)

    def stage_1(i):
        @pl.when(i >= 2)
        def _():
            at_1(i - 2).wait_send()

        at_c(i).wait_recv()
        away = pl.ds(aligned((1 - b1) * fourth), fourth)
        send_1[i % 2] = (own_c[:, away] + recv_c[i, :, away].astype(F32)).astype(BF16)
        at_1(i).start()
        kept = pl.ds(aligned(b1 * fourth), fourth)
        own_1[...] = own_c[:, kept] + recv_c[i, :, kept].astype(F32)

    def stage_2(i):
        @pl.when(i >= 2)
        def _():
            at_2(i - 2).wait_send()

        at_1(i).wait_recv()
        away = pl.ds(aligned((1 - b2) * eighth), eighth)
        send_2[i % 2] = (own_1[:, away] + recv_1[i, :, away].astype(F32)).astype(BF16)
        at_2(i).start()
        kept = pl.ds(aligned(b2 * eighth), eighth)
        own_2[...] = own_1[:, kept] + recv_1[i, :, kept].astype(F32)

    def stage_3(i):
        at_2(i).wait_recv()
        merged[rows_of(i), pl.ds(aligned(off_2), eighth)] = (own_2[...] + recv_2[i].astype(F32)).astype(BF16)
        back_2(i).start()

    def stage_4(i):
        back_2(i).wait_recv()
        back_1(i).start()

    def stage_5(i):
        back_1(i).wait_recv()
        back_c(i).start()

    def gather_add(i):
        back_c(i).wait_recv()
        left = patch[:, :, pl.ds(aligned(i * ROWS, ROWS), ROWS)].reshape(n_t * rows, ROWS)

        def one(j, carry):
            at = pl.ds(aligned(j * tile, tile), tile)
            value = jnp.dot(left, merged[rows_of(i), at], preferred_element_type=F32)

            @pl.when(i == 0)
            def _():
                total[:, at] = value

            @pl.when(i > 0)
            def _():
                total[:, at] += value

            return carry

        lax.fori_loop(0, wide // tile, one, 0)

    def square_send(k):
        to = (z + k) % n_t
        return remote(squares.at[to], squares_in.at[z], sq_s.at[k - 1], sq_r.at[k - 1], (dp, to, y))

    def factor_send(k):
        return remote(factor, factor_in.at[z], fa_s.at[k - 1], fa_r.at[k - 1], (dp, (z + k) % n_t, y))

    def embed():
        for t in range(n_t):
            lanes = jnp.zeros((rows, 128), F32)
            for d in range(quarter.shape[0]):
                value = jnp.dot(patch[t], quarter[d], preferred_element_type=F32).astype(BF16)
                emb[t, :, d * duo : (d + 1) * duo] = value
                value = value.astype(F32)
                value = value * value
                for e in range(duo // 128):
                    lanes = lanes + value[:, e * 128 : (e + 1) * 128]
            squares[t] = lanes
        squares_in[z] = squares[z]
        for k in range(1, n_t):
            square_send(k).start()

    def row_factor():
        for k in range(1, n_t):
            square_send(k).wait_recv()
        lanes = squares_in[0]
        for t in range(1, n_t):
            lanes = lanes + squares_in[t]
        mean = jnp.sum(lanes, axis=-1, keepdims=True) * (1.0 / D)
        factor[...] = jnp.broadcast_to(lax.rsqrt(mean + eps), factor.shape)
        factor_in[z] = factor[...]
        for k in range(1, n_t):
            factor_send(k).start()

    def own_action_rows():
        for m in range(1, 8):
            apart_send(m).wait_recv()
        value = apart_in[0].astype(F32)
        for g in range(1, 8):
            value = value + apart_in[g].astype(F32)
        qkv_act[...] = value.astype(BF16)

    me_1 = dev_1[0] * 2 + dev_1[2]
    me_2 = dev_2[0] * 2 + dev_2[2]
    me_12 = dp_x * 2 + y_n
    lineage = (me, me_1, me_2, me_12)

    def wo_core(k):
        block = wo_ref.at[lineage[k]]
        return remote(block, block, wo_s.at[k], wo_r.at[k], dev_c)

    def wo_first():
        block = wo_ref.at[me]
        return remote(block, block, wo_s.at[4], wo_r.at[4], dev_1)

    def wo_second(k):
        block = wo_ref.at[lineage[k]]
        return remote(block, block, wo_s.at[5 + k], wo_r.at[5 + k], dev_2)

    spread(0)

    def step(s, carry):
        @pl.when(s < chunks - 1)
        def _():
            spread(s + 1)

        for g in range(3):
            @pl.when(s == 2 * g)
            def _():
                for k in range(1, n_t):
                    patch_send(k, g).start()

        @pl.when(s < chunks)
        def _():
            stage_c(s)

        @pl.when((s >= 1) & (s <= chunks))
        def _():
            stage_2(s - 1)

        @pl.when((s >= 2) & (s <= chunks + 1))
        def _():
            stage_4(s - 2)

        @pl.when(s < chunks)
        def _():
            stage_1(s)

        @pl.when((s >= 1) & (s <= chunks))
        def _():
            stage_3(s - 1)

        @pl.when((s >= 2) & (s <= chunks + 1))
        def _():
            stage_5(s - 2)

        @pl.when(s == 1)
        def _():
            loads[6].wait()
            wo_core(0).start()
            own_action_rows()

        @pl.when(s == 2)
        def _():
            proj_x().wait_recv()

        for g in range(3):
            @pl.when(s == 2 * g + 3)
            def _():
                for k in range(1, n_t):
                    patch_send(k, g).wait_recv()

        @pl.when(s >= 3)
        def _():
            gather_add(s - 3)

        @pl.when(s == chunks - 2)
        def _():
            proj_diag().start()
            proj_core(0).start()

        @pl.when(s == chunks - 1)
        def _():
            proj_diag().wait_recv()
            proj_core(1).start()

        @pl.when(s == chunks)
        def _():
            proj_core(0).wait_recv()
            proj_core(1).wait_recv()
            embed()

        @pl.when(s == chunks + 1)
        def _():
            wo_first().start()
            row_factor()

        return carry

    lax.fori_loop(0, chunks + 3, step, 0)

    for k in range(1, n_t):
        factor_send(k).wait_recv()

    def scale_tile(j, carry):
        at = pl.ds(aligned(j * tile, tile), tile)
        for t in range(n_t):
            for f in range(frames):
                piece = pl.ds(t * rows + f * local, local)
                value = total[piece, at] * factor_in[t, f * local : (f + 1) * local, 0:1]
                qkv[f, t * local : (t + 1) * local, at] = value.astype(BF16)
        return carry

    lax.fori_loop(0, wide // tile, scale_tile, 0)

    inv_root = 1.0 / math.sqrt(HD)
    length = n_t * local
    nt = (((1,), (1,)), ((), ()))
    causal = lax.broadcasted_iota(jnp.int32, (length, length), 0) >= lax.broadcasted_iota(
        jnp.int32, (length, length), 1
    )
    slot_i = lax.broadcasted_iota(jnp.int32, (slots, slots), 0)
    slot_j = lax.broadcasted_iota(jnp.int32, (slots, slots), 1)
    slot_sees = (slot_i // SLOTS == slot_j // SLOTS) & (slot_i >= slot_j)
    slot_frame = lax.broadcasted_iota(jnp.int32, (slots, HD), 0) // SLOTS

    def one_head(h, carry):
        qc, kc, vc = (pl.ds(aligned(part_at * width + h * HD), HD) for part_at in range(3))
        qa, ka, va = qkv_act[:, qc], qkv_act[:, kc], qkv_act[:, vc]
        near = lax.dot_general(qa, ka, nt, preferred_element_type=F32) * inv_root
        near = jnp.where(slot_sees, near, -1e30)
        mixed_slots = jnp.zeros((slots, HD), F32)
        for f in range(frames):
            q, k, v = qkv[f, :, qc], qkv[f, :, kc], qkv[f, :, vc]
            scores = lax.dot_general(q, k, nt, preferred_element_type=F32) * inv_root
            scores = jnp.where(causal, scores, -1e30)
            scores = jnp.exp(scores - jnp.max(scores, axis=-1, keepdims=True))
            scores = scores / jnp.sum(scores, axis=-1, keepdims=True)
            value = jnp.dot(scores.astype(BF16), v, preferred_element_type=F32).astype(BF16)
            for t in range(n_t):
                mixed[t, f * local : (f + 1) * local, pl.ds(aligned(h * HD), HD)] = value[t * local : (t + 1) * local]
            far = lax.dot_general(qa, k, nt, preferred_element_type=F32) * inv_root
            top = jnp.maximum(jnp.max(far, axis=-1, keepdims=True), jnp.max(near, axis=-1, keepdims=True))
            far, close = jnp.exp(far - top), jnp.exp(near - top)
            below = jnp.sum(far, axis=-1, keepdims=True) + jnp.sum(close, axis=-1, keepdims=True)
            value = jnp.dot((far / below).astype(BF16), v, preferred_element_type=F32)
            value = value + jnp.dot((close / below).astype(BF16), va, preferred_element_type=F32)
            mixed_slots = jnp.where(slot_frame == f, value, mixed_slots)
        mixed_act[:, pl.ds(aligned(h * HD), HD)] = mixed_slots.astype(BF16)
        return carry

    lax.fori_loop(0, heads, one_head, 0)

    wo_first().wait_recv()
    wo_core(1).start()
    wo_second(0).start()
    wo_second(1).start()

    def block_of(j, e):
        xs, ys = ((x, y), (x, y), (1 - x, y), (x, 1 - y), (x, 1 - y), (1 - x, y), (1 - x, 1 - y), (1 - x, 1 - y))[
            2 * j + e
        ]
        return 4 * xs + 2 * e + ys

    def contribution(t, j):
        left = mixed[t]
        for e in range(2):
            g = block_of(j, e)
            part[:, e * depth : (e + 1) * depth] = jnp.dot(left, wo_ref[g], preferred_element_type=F32)

            @pl.when(z // pairs == g % 2)
            def _():
                at = pl.ds(aligned(e * depth + (z % pairs) * duo), duo)
                part[:, at] += emb[t, :, pl.ds(aligned((g // 2) * duo), duo)].astype(F32)

    line = n_t - 1

    def to_right(n):
        return remote(right_out.at[n % 4], right_in.at[n], rr_s.at[n], rr_r.at[n], (dp, lax.rem(z + 1, n_t), y))

    def to_left(n):
        return remote(left_out.at[n % 4], left_in.at[n], rl_s.at[n], rl_r.at[n], (dp, lax.rem(z + n_t - 1, n_t), y))

    def aup_send(j):
        return remote(aup.at[j], aup_in.at[z], au_s.at[j], au_r.at[z], (dp, j, y))

    def finish(j):
        contribution(z, j)

        @pl.when(z > 0)
        def _():
            n = j * line + line - z
            to_right(n).wait_recv()
            part[...] += right_in[n].astype(F32)

        @pl.when(z < n_t - 1)
        def _():
            n = j * line + z
            to_left(n).wait_recv()
            part[...] += left_in[n].astype(F32)

        for e in range(2):
            at = pl.ds(aligned(block_of(j, e) * depth, depth), depth)
            out_ref[:, at] = part[:, e * depth : (e + 1) * depth].astype(BF16)

    for j in range(4):
        if j == 0:
            wo_core(0).wait_recv()
        elif j == 1:
            wo_core(1).wait_recv()
        elif j == 2:
            wo_second(0).wait_recv()
            wo_core(2).start()
            wo_second(1).wait_recv()
            wo_core(3).start()
            wo_core(2).wait_recv()
        else:
            wo_core(3).wait_recv()

        def shift(m, carry):
            n = j * line + m
            t = line - m

            @pl.when((n >= 4) & (z < line - (n - 4) % line))
            def _():
                to_right(n - 4).wait_send()

            @pl.when((n >= 4) & (z > (n - 4) % line))
            def _():
                to_left(n - 4).wait_send()

            @pl.when(z < t)
            def _():
                contribution(t, j)

                @pl.when(z > 0)
                def _():
                    to_right(n).wait_recv()
                    part[...] += right_in[n].astype(F32)

                right_out[n % 4] = part[...].astype(BF16)
                to_right(n).start()

            @pl.when(z > m)
            def _():
                contribution(m, j)

                @pl.when(z < line)
                def _():
                    to_left(n).wait_recv()
                    part[...] += left_in[n].astype(F32)

                left_out[n % 4] = part[...].astype(BF16)
                to_left(n).start()

            return carry

        lax.fori_loop(0, line, shift, 0)
        for e in range(2):
            aup[j, :, e * depth : (e + 1) * depth] = jnp.dot(
                mixed_act[...], wo_ref[block_of(j, e)], preferred_element_type=F32
            ).astype(BF16)

        @pl.when(z != j)
        def _():
            aup_send(j).start()

        @pl.when(z == j)
        def _():
            for e in range(2):
                pltpu.make_async_copy(
                    head_hbm.at[pl.ds(aligned(block_of(j, e) * depth, depth), depth)],
                    head.at[pl.ds(e * depth, depth)],
                    local_sem.at[7 + e],
                ).start()

        if j > 0:
            finish(j - 1)
    finish(3)

    def asq_send(k):
        return remote(asq, asq_in.at[z], aq_s.at[k - 1], aq_r.at[k - 1], (dp, (z + k) % n_t, y))

    def alog_send(k):
        return remote(alog, alog_in.at[z], al_s.at[k - 1], al_r.at[k - 1], (dp, (z + k) % n_t, y))

    for j in range(4):
        @pl.when(z == j)
        def _():
            aup_in[j] = aup[j]
            for t in range(n_t):
                if t != j:
                    remote(aup.at[j], aup_in.at[t], au_s.at[j], au_r.at[t], (dp, j, y)).wait_recv()
            value = aup_in[0].astype(F32)
            for t in range(1, n_t):
                value = value + aup_in[t].astype(F32)
            gains = []
            lanes = jnp.zeros((slots, 128), F32)
            for e in range(2):
                at = pl.ds(aligned(block_of(j, e) * depth, depth), depth)
                acted = value[:, e * depth : (e + 1) * depth] + act[:, at]
                part[0:slots, e * depth : (e + 1) * depth] = acted
                part[slots : 2 * slots, e * depth : (e + 1) * depth] = jnp.broadcast_to(
                    final_gain_ref[:, at].astype(F32), (slots, depth)
                )
                for q in range(depth // 128):
                    piece = acted[:, q * 128 : (q + 1) * 128]
                    lanes = lanes + piece * piece
            asq[...] = lanes

    asq_in[z] = asq[...]
    for k in range(1, n_t):
        asq_send(k).start()
    for e in range(2):
        pltpu.make_async_copy(
            head_hbm.at[pl.ds(0, depth)], head.at[pl.ds(e * depth, depth)], local_sem.at[7 + e]
        ).wait()
    for k in range(1, n_t):
        asq_send(k).wait_recv()
    lanes = asq_in[0]
    for t in range(1, n_t):
        lanes = lanes + asq_in[t]
    scale = lax.rsqrt(jnp.sum(lanes, axis=-1, keepdims=True) * (1.0 / D) + eps)
    final = (part[0:slots, :] * scale * part[slots : 2 * slots, :]).astype(BF16)
    alog[...] = jnp.dot(final, head[...], preferred_element_type=F32)
    alog_in[z] = alog[...]
    for k in range(1, n_t):
        alog_send(k).start()
    for k in range(1, n_t):
        alog_send(k).wait_recv()
    logits = alog_in[0]
    for t in range(1, n_t):
        logits = logits + alog_in[t]
    picked = jnp.sum(logits * chosen_ref[...], axis=-1, keepdims=True)
    top = jnp.max(logits, axis=-1, keepdims=True)
    spread_out = jnp.log(jnp.sum(jnp.exp(logits - top), axis=-1, keepdims=True)) + top
    loss_ref[...] = jnp.broadcast_to(spread_out - picked, loss_ref.shape)

    for i in range(chunks):
        proj_y(i).wait_send()
        back_2(i).wait_send()
        back_1(i).wait_send()
        back_c(i).wait_send()
        spread_done(i)
    for i in range(chunks - 2, chunks):
        at_c(i).wait_send()
        at_1(i).wait_send()
        at_2(i).wait_send()
    proj_x().wait_send()
    proj_diag().wait_send()
    for k in range(2):
        proj_core(k).wait_send()
    for m in range(1, 8):
        act_send(m).wait_send()
        apart_send(m).wait_send()
    for k in range(1, n_t):
        for g in range(3):
            patch_send(k, g).wait_send()
        square_send(k).wait_send()
        factor_send(k).wait_send()
        asq_send(k).wait_send()
        alog_send(k).wait_send()
    for k in range(4):
        wo_core(k).wait_send()
    wo_first().wait_send()
    wo_second(0).wait_send()
    wo_second(1).wait_send()
    for n in range(4 * line - 4, 4 * line):
        @pl.when(z < line - n % line)
        def _():
            to_right(n).wait_send()

        @pl.when(z > n % line)
        def _():
            to_left(n).wait_send()
    for j in range(4):
        @pl.when(z != j)
        def _():
            aup_send(j).wait_send()


def fits(mesh, patches, proj_w, wq, wo):
    frames, local, vision = patches.shape
    n_t = mesh.shape["tensor"]
    return (
        mesh.shape["dp"] == 4
        and mesh.shape["section"] == 2
        and n_t == 4
        and proj_w.shape[1] % 128 == 0
        and 8 * wq.shape[0] == D
        and n_t * wq.shape[1] == D
        and vision % (3 * ROWS) == 0
        and local % 16 == 0
        and frames * SLOTS % 16 == 0
    )


def program(
    mesh, patches, teacher, proj_w, norm_gain, wq, wk, wv, wo, start_row, action_table, final_gain, head_w
):
    if not fits(mesh, patches, proj_w, wq, wo):
        return on_device(
            patches, teacher, proj_w, norm_gain, wq, wk, wv, wo, start_row, action_table, final_gain, head_w
        )
    frames, local, vision = patches.shape
    n_t = mesh.shape["tensor"]
    rows, slots = frames * local, frames * SLOTS
    depth, width = wq.shape
    cols = proj_w.shape[1]
    wide, chunks, pairs, line = 3 * width, vision // ROWS, n_t // 2, n_t - 1
    none = jnp.full((frames, 1), -1, jnp.int32)
    bins = jnp.arange(BINS, dtype=jnp.int32)
    lookup = (jnp.concatenate([none, teacher], axis=1)[..., None] == bins).astype(BF16).reshape(slots, BINS)
    chosen = (jnp.concatenate([teacher, none], axis=1)[..., None] == bins).astype(F32).reshape(slots, BINS)
    vmem, anywhere = pl.BlockSpec(memory_space=pltpu.VMEM), pl.BlockSpec(memory_space=pl.ANY)
    dma = pltpu.SemaphoreType.DMA
    scratch = [
        pltpu.VMEM((depth, wide), BF16),
        pltpu.VMEM((8,) + wo.shape, BF16),
        pltpu.VMEM((4, vision, 2 * cols), BF16),
        pltpu.VMEM((pairs, vision, 2 * cols), BF16),
        pltpu.VMEM((n_t, rows, vision), BF16),
        pltpu.VMEM(action_table.shape, BF16),
        pltpu.VMEM((2 * depth, BINS), BF16),
        pltpu.VMEM((2, ROWS, wide // 2), BF16),
        pltpu.VMEM((chunks, ROWS, wide // 2), BF16),
        pltpu.VMEM((2, ROWS, wide // 4), BF16),
        pltpu.VMEM((chunks, ROWS, wide // 4), BF16),
        pltpu.VMEM((2, ROWS, wide // 8), BF16),
        pltpu.VMEM((chunks, ROWS, wide // 8), BF16),
        pltpu.VMEM((ROWS, wide // 2), F32),
        pltpu.VMEM((ROWS, wide // 4), F32),
        pltpu.VMEM((ROWS, wide // 8), F32),
        pltpu.VMEM((vision, wide), BF16),
        pltpu.VMEM((n_t * rows, wide), F32),
        pltpu.VMEM((frames, n_t * local, wide), BF16),
        pltpu.VMEM((n_t, rows, width), BF16),
        pltpu.VMEM((n_t, rows, 8 * cols), BF16),
        pltpu.VMEM((n_t, rows, 128), F32),
        pltpu.VMEM((n_t, rows, 128), F32),
        pltpu.VMEM((rows, 128), F32),
        pltpu.VMEM((n_t, rows, 128), F32),
        pltpu.VMEM((slots, D), F32),
        pltpu.VMEM((slots, D), BF16),
        pltpu.VMEM((8, slots, depth), BF16),
        pltpu.VMEM((8, slots, wide), BF16),
        pltpu.VMEM((8, slots, wide), BF16),
        pltpu.VMEM((slots, wide), BF16),
        pltpu.VMEM((slots, width), BF16),
        pltpu.VMEM((n_t, slots, 2 * depth), BF16),
        pltpu.VMEM((n_t, slots, 2 * depth), BF16),
        pltpu.VMEM((slots, 128), F32),
        pltpu.VMEM((n_t, slots, 128), F32),
        pltpu.VMEM((slots, BINS), F32),
        pltpu.VMEM((n_t, slots, BINS), F32),
        pltpu.VMEM((4, rows, 2 * depth), BF16),
        pltpu.VMEM((4, rows, 2 * depth), BF16),
        pltpu.VMEM((4 * line, rows, 2 * depth), BF16),
        pltpu.VMEM((4 * line, rows, 2 * depth), BF16),
        pltpu.VMEM((rows, 2 * depth), F32),
        dma((9,)),
        dma((chunks,)), dma((chunks,)),
        dma, dma, dma, dma,
        dma((2,)), dma((2,)),
        dma((pairs, chunks)), dma((pairs, chunks)), dma((pairs, chunks)),
        dma((line, 3)), dma((line, 3)),
        dma((7,)), dma((7,)), dma((7,)), dma((7,)),
    ]
    scratch += [dma((chunks,))] * 12
    scratch += [dma((line,))] * 4
    scratch += [dma((7,))] * 2
    scratch += [dma((4 * line,))] * 4
    scratch += [dma((n_t,))] * 2 + [dma((line,))] * 4
    hidden, loss = pl.pallas_call(
        functools.partial(fused, (n_t, frames, local)),
        out_shape=(
            jax.ShapeDtypeStruct((rows, D), BF16),
            jax.ShapeDtypeStruct((slots, 128), F32),
        ),
        in_specs=[vmem] * 5 + [anywhere] * 8,
        out_specs=(vmem, vmem),
        scratch_shapes=scratch,
        compiler_params=pltpu.CompilerParams(
            collective_id=0, has_side_effects=True, vmem_limit_bytes=67043328
        ),
    )(
        norm_gain.reshape(1, D),
        start_row.reshape(1, D),
        final_gain.reshape(1, D),
        lookup,
        chosen,
        patches.reshape(rows, vision),
        proj_w,
        wq,
        wk,
        wv,
        wo,
        action_table,
        head_w,
    )
    return hidden.reshape(frames, local, D), loss[:, 0].reshape(frames, SLOTS)[:, :ADIM]


def solution(mesh):
    return jax.shard_map(
        functools.partial(program, mesh),
        mesh=mesh,
        in_specs=(
            P(("dp", "section"), "tensor", None),
            P(("dp", "section"), None),
            P(None, ("dp", "tensor", "section")),
            P(),
            P(("dp", "section"), "tensor"),
            P(("dp", "section"), "tensor"),
            P(("dp", "section"), "tensor"),
            P("tensor", ("dp", "section")),
            P(),
            P(),
            P(),
            P(),
        ),
        out_specs=(P(("dp", "section"), "tensor", None), P(("dp", "section"), None)),
        check_vma=False,
    )
```

```python
import functools
import math

import jax
import jax.numpy as jnp
from jax import lax
from jax.experimental import pallas as pl
from jax.experimental.pallas import tpu as pltpu
from jax.sharding import PartitionSpec as P

D = 4096
HD = 128
V = 1152
P_SIZE = 256
BINS = 256
ADIM = 7
SLOTS = 8


eps = 1e-05


def normalize(rows, gain):
    rows = rows.astype(jnp.float32)
    factor = lax.rsqrt(jnp.mean(rows * rows, axis=-1, keepdims=True) + eps)
    return rows * factor * gain.astype(jnp.float32)


def action_rows(teacher, start_row, action_table):
    frames = teacher.shape[0]
    onehot = (teacher[..., None] == jnp.arange(BINS, dtype=jnp.int32)).astype(jnp.bfloat16)
    looked = jnp.dot(onehot.reshape(-1, BINS), action_table, preferred_element_type=jnp.float32)
    looked = looked.astype(jnp.bfloat16).reshape(frames, ADIM, D)
    start = jnp.broadcast_to(start_row.reshape(1, 1, D), (frames, 1, D))
    return jnp.concatenate([start, looked], axis=1)


def line_gather(own, axis):
    n = lax.axis_size(axis)
    here = lax.axis_index(axis)
    right = left = own
    from_left, from_right = [], []
    for r in range(n - 1):
        right = lax.ppermute(right, axis, [(t, t + 1) for t in range(r, n - 1)])
        left = lax.ppermute(left, axis, [(t, t - 1) for t in range(1, n - r)])
        from_left.append(right)
        from_right.append(left)
    blocks = jnp.zeros((n,) + own.shape, own.dtype)
    blocks = lax.dynamic_update_index_in_dim(blocks, own, here, 0)
    for r in range(n - 1):
        block = jnp.where(here > r, from_left[r], from_right[n - 2 - r])
        blocks = lax.dynamic_update_index_in_dim(blocks, block, lax.rem(here - 1 - r + n, n), 0)
    return blocks


def line_reduce_scatter(parts, axis):
    n = lax.axis_size(axis)
    here = lax.axis_index(axis)

    def part(c):
        return lax.dynamic_index_in_dim(parts, jnp.clip(c, 0, n - 1), 0, keepdims=False)

    right = left = None
    for r in range(n - 1):
        steps = range(min(r, n - 2) + 1)
        to_right = part(n - 1 - r + here)
        to_left = part(r - (n - 1) + here)
        if right is not None:
            to_right = to_right + right.astype(jnp.float32)
            to_left = to_left + left.astype(jnp.float32)
        right = lax.ppermute(to_right.astype(jnp.bfloat16), axis, [(t, t + 1) for t in steps])
        left = lax.ppermute(
            to_left.astype(jnp.bfloat16), axis, [(n - 1 - t, n - 2 - t) for t in steps]
        )
    total = part(here)
    if right is not None:
        total = total + right.astype(jnp.float32) + left.astype(jnp.float32)
    return total


def plane_columns(own):
    rows, columns = own.shape
    blocks = line_gather(line_gather(own, "section").reshape(-1, columns), "dp")
    blocks = blocks.reshape(-1, rows, columns)
    return jnp.concatenate([blocks[i] for i in range(blocks.shape[0])], axis=1)


RELAYS = 2


def on_device(
    patches, teacher, proj_w, norm_gain, wq, wk, wv, wo, start_row, action_table, final_gain, head_w
):
    frames = patches.shape[0]
    local_patches = patches.shape[1]
    length = P_SIZE + SLOTS
    plane = ("dp", "section")
    n_dp, n_t = lax.axis_size("dp"), lax.axis_size("tensor")
    here = lax.axis_index("tensor")
    proj_part = plane_columns(proj_w)
    all_patches = line_gather(patches.reshape(-1, V), "tensor")
    all_patches = all_patches.reshape(n_t, frames, local_patches, V).transpose(1, 0, 2, 3)
    embedded_part = jnp.dot(
        all_patches.reshape(-1, V), proj_part, preferred_element_type=jnp.float32
    ).astype(jnp.bfloat16)
    blocks = line_gather(embedded_part, "tensor")
    width = embedded_part.shape[1] // n_dp
    embedded_all = jnp.concatenate(
        [blocks[t, :, d * width : (d + 1) * width] for d in range(n_dp) for t in range(n_t)], axis=1
    ).reshape(frames, P_SIZE, D)
    embedded_own = lax.dynamic_slice_in_dim(embedded_all, here * local_patches, local_patches, 1)
    actions = action_rows(teacher, start_row, action_table)
    stream = jnp.concatenate([embedded_all, actions], axis=1)
    normed = normalize(stream, norm_gain).astype(jnp.bfloat16).reshape(-1, D)
    full_out = plane_columns(wo)
    local_width = wq.shape[1]
    projected = tuple(
        jnp.dot(
            normed,
            lax.all_gather(weight, plane, axis=0, tiled=True),
            preferred_element_type=jnp.float32,
        )
        for weight in (wq, wk, wv)
    )
    heads_local = local_width // HD
    queries, keys_all, values_all = [
        part.astype(jnp.bfloat16).reshape(frames, length, heads_local, HD) for part in projected
    ]
    inv_root = 1.0 / math.sqrt(HD)
    scores = (
        jnp.einsum("fqhd,fkhd->fhqk", queries, keys_all, preferred_element_type=jnp.float32)
        * inv_root
    )
    positions = jnp.arange(length, dtype=jnp.int32)
    causal = positions[:, None] >= positions[None, :]
    scores = jnp.where(causal[None, None], scores, -1e30)
    weights = jax.nn.softmax(scores, axis=-1).astype(jnp.bfloat16)
    mixed = jnp.einsum("fhqk,fkhd->fqhd", weights, values_all, preferred_element_type=jnp.float32)
    mixed = mixed.astype(jnp.bfloat16).reshape(frames, length, local_width)
    patch_rows = mixed[:, :P_SIZE].reshape(frames, n_t, local_patches, local_width)
    patch_rows = patch_rows.transpose(1, 0, 2, 3).reshape(n_t, -1, local_width)
    slot_rows = mixed[:, P_SIZE:].reshape(-1, local_width)
    slot_part = jnp.dot(slot_rows, full_out, preferred_element_type=jnp.float32)
    slot_parts = line_gather(slot_part.astype(jnp.bfloat16), "tensor")
    slot_update = jnp.sum(slot_parts.astype(jnp.float32), axis=0)
    chunk = D // RELAYS
    updates = []
    for j in range(RELAYS):
        parts = jnp.einsum(
            "nrw,wc->nrc",
            patch_rows,
            full_out[:, j * chunk : (j + 1) * chunk],
            preferred_element_type=jnp.float32,
        )
        updates.append(line_reduce_scatter(parts, "tensor"))
    update = jnp.concatenate(updates, axis=1).reshape(frames, local_patches, D)
    hidden_out = (embedded_own.astype(jnp.float32) + update).astype(jnp.bfloat16)
    acted = (actions.astype(jnp.float32) + slot_update.reshape(frames, SLOTS, D))[:, :ADIM]
    final = normalize(acted, final_gain).astype(jnp.bfloat16).reshape(-1, D)
    logits = jnp.dot(final, head_w, preferred_element_type=jnp.float32).reshape(frames, ADIM, BINS)
    chosen = (teacher[..., None] == jnp.arange(BINS, dtype=jnp.int32)).astype(jnp.float32)
    picked = jnp.sum(logits * chosen, axis=-1)
    loss = jax.nn.logsumexp(logits, axis=-1) - picked
    return (hidden_out, loss)


MESH = pl.DeviceIdType.MESH
ROWS = 128
F32 = jnp.float32
BF16 = jnp.bfloat16


def aligned(value, to=128):
    return pl.multiple_of(value, to)


def fused(
    sizes,
    teacher_ref, rows_hbm,
    patches_hbm, proj_hbm, wq_hbm, wk_hbm, wv_hbm, wo_hbm, table_hbm, head_hbm,
    out_hbm, loss_ref,
    rows_ref, w_ref, wo_ref, quarter, pair, patch, table, head,
    send_c, recv_c, send_1, recv_1, send_2, recv_2, own_c, own_1, own_2, merged,
    total, qkv, mixed, emb, squares, squares_in, factor, factor_in,
    act, nact, nact_all, apart, apart_in_c, apart_two, apart_in_1, apart_one, apart_in_2, qkv_act, mixed_act, aup, aup_in, asq, asq_in, alog, alog_in,
    stage, acted, right_out, left_out, right_in, left_in, part,
    local_sem, py_s, py_r, px_s, px_r, pd_s, pd_r, pc_s, pc_r, zr_s, zl_s, z_r, zd_s,
    pz_s, pz_r, na_s, na_r, ap_s, ap_r, c_s, c_r, s1_s, s1_r, s2_s, s2_r, g2_s, g2_r, g1_s, g1_r, gc_s, gc_r,
    sq_s, sq_r, fa_s, fa_r, wo_s, wo_r, wf_s, wf_r, rr_s, rr_r, rl_s, rl_r, au_s, au_r, aq_s, aq_r, al_s, al_r,
):
    n_t, frames, local = sizes
    dp, z, y = lax.axis_index("dp"), lax.axis_index("tensor"), lax.axis_index("section")
    c, x = dp % 2, dp // 2
    me = dp * 2 + y
    place = c * 4 + x * 2 + y
    dp_x, dp_c, y_n = dp + 2 - 4 * x, dp + 1 - 2 * c, 1 - y
    dev_1 = (dp + (1 - c) * (2 - 4 * x), z, y + c * (1 - 2 * y))
    dev_2 = (dp + c * (2 - 4 * x), z, y + (1 - c) * (1 - 2 * y))
    dev_c, dev_x, dev_y = (dp_c, z, y), (dp_x, z, y), (dp, z, y_n)
    b1, b2 = (1 - c) * x + c * y, (1 - c) * y + c * x
    rows = frames * local
    depth, width = wq_hbm.shape
    cols = proj_hbm.shape[1]
    vision = proj_hbm.shape[0]
    chunks = vision // ROWS
    wide = 3 * width
    half, fourth, eighth = wide // 2, wide // 4, wide // 8
    pairs = n_t // 2
    duo = 2 * cols
    heads = width // HD

    def remote(src, dst, send, recv, device):
        return pltpu.make_async_remote_copy(
            src_ref=src, dst_ref=dst, send_sem=send, recv_sem=recv, device_id=device, device_id_type=MESH
        )

    def plane_peer(m):
        g = (me + m) % 8
        return g, (g // 2, z, g % 2)

    own_col = aligned(y * cols, cols)
    loads = [
        pltpu.make_async_copy(proj_hbm, quarter.at[dp, :, pl.ds(own_col, cols)], local_sem.at[0]),
        pltpu.make_async_copy(patches_hbm, patch.at[z], local_sem.at[1]),
        pltpu.make_async_copy(table_hbm, table, local_sem.at[2]),
        pltpu.make_async_copy(wq_hbm, w_ref.at[:, pl.ds(0, width)], local_sem.at[3]),
        pltpu.make_async_copy(wk_hbm, w_ref.at[:, pl.ds(width, width)], local_sem.at[4]),
        pltpu.make_async_copy(wv_hbm, w_ref.at[:, pl.ds(2 * width, width)], local_sem.at[5]),
        pltpu.make_async_copy(wo_hbm, wo_ref.at[me], local_sem.at[6]),
        pltpu.make_async_copy(rows_hbm, rows_ref, local_sem.at[9]),
    ]
    for load in loads:
        load.start()

    barrier = pltpu.get_barrier_semaphore()
    for m in range(1, 8):
        pl.semaphore_signal(barrier, inc=1, device_id=plane_peer(m)[1], device_id_type=MESH)
    for k in range(1, n_t):
        pl.semaphore_signal(barrier, inc=1, device_id=(dp, (z + k) % n_t, y), device_id_type=MESH)
    pl.semaphore_wait(barrier, 7 + n_t - 1)

    def rows_of(i):
        return pl.ds(aligned(i * ROWS, ROWS), ROWS)

    def proj_y(i):
        block = quarter.at[dp, rows_of(i), pl.ds(own_col, cols)]
        return remote(block, block, py_s.at[i], py_r.at[i], dev_y)

    def proj_x():
        block = quarter.at[dp, :, pl.ds(own_col, cols)]
        return remote(block, block, px_s, px_r, dev_x)

    def proj_diag():
        at = dp * (1 - c) + dp_x * c
        col = aligned(((1 - c) * (1 - y) + c * y) * cols, cols)
        block = quarter.at[at, :, pl.ds(col, cols)]
        return remote(block, block, pd_s, pd_r, dev_1)

    def proj_core(k):
        block = quarter.at[(dp, dp_x)[k]]
        return remote(block, block, pc_s.at[k], pc_r.at[k], dev_c)

    def patch_send(k, i):
        block = patch.at[z, :, pl.ds(aligned(i * ROWS, ROWS), ROWS)]
        return remote(block, block, pz_s.at[k - 1, i], pz_r.at[k - 1, i], (dp, (z + k) % n_t, y))

    def act_send(m):
        g, device = plane_peer(m)
        col = aligned(g * depth, depth)
        return remote(nact.at[:, pl.ds(col, depth)], nact_all.at[place], na_s.at[m - 1], na_r.at[m - 1], device)

    def apart_c():
        return remote(apart.at[pl.ds((1 - c) * 4, 4)], apart_in_c, ap_s.at[0], ap_r.at[0], dev_c)

    def apart_1():
        return remote(apart_two.at[pl.ds((1 - b1) * 2, 2)], apart_in_1, ap_s.at[1], ap_r.at[1], dev_1)

    def apart_2():
        return remote(apart_one.at[1 - b2], apart_in_2, ap_s.at[2], ap_r.at[2], dev_2)

    def z_right(p, i, own):
        src = quarter.at[dp, rows_of(i)] if own else pair.at[p, rows_of(i)]
        return remote(src, pair.at[p, rows_of(i)], zr_s.at[p, i], z_r.at[p, i], (dp, lax.rem(z + 1, n_t), y))

    def z_left(p, i, own):
        src = quarter.at[dp, rows_of(i)] if own else pair.at[p, rows_of(i)]
        return remote(src, pair.at[p, rows_of(i)], zl_s.at[p, i], z_r.at[p, i], (dp, lax.rem(z + n_t - 1, n_t), y))

    def z_first(p, k):
        block = quarter.at[dp, rows_of(0)]
        return remote(block, pair.at[p, rows_of(0)], zd_s.at[k - 1], z_r.at[p, 0], (dp, (z + k) % n_t, y))

    def first_pair():
        proj_y(0).wait_recv()
        for p in range(pairs):
            @pl.when(z == pairs * y + p)
            def _():
                for k in range(1, n_t):
                    z_first(p, k).start()
                pair[p, rows_of(0)] = quarter[dp, rows_of(0)]

    def first_spread():
        for p in range(pairs):
            @pl.when(z != pairs * y + p)
            def _():
                z_first(p, 1).wait_recv()

    def own_pair(i):
        for p in range(pairs):
            @pl.when(z == pairs * y + p)
            def _():
                @pl.when(z < n_t - 1)
                def _():
                    z_right(p, i, True).start()

                @pl.when(z > 0)
                def _():
                    z_left(p, i, True).start()

                pair[p, rows_of(i)] = quarter[dp, rows_of(i)]

    def spread(i):
        for p in range(pairs):
            home = pairs * y + p

            @pl.when(z > home)
            def _():
                z_right(p, i, False).wait_recv()

                @pl.when(z < n_t - 1)
                def _():
                    z_right(p, i, False).start()

            @pl.when(z < home)
            def _():
                z_left(p, i, False).wait_recv()

                @pl.when(z > 0)
                def _():
                    z_left(p, i, False).start()

    loads[0].wait()
    for i in range(chunks):
        proj_y(i).start()
    proj_x().start()
    loads[7].wait()

    slots = frames * SLOTS
    row_at = lax.broadcasted_iota(jnp.int32, (slots, BINS), 0)
    bin_at = lax.broadcasted_iota(jnp.int32, (slots, BINS), 1)

    def one_hot(first):
        index = jnp.full((slots, BINS), -1, jnp.int32)
        for f in range(frames):
            for a in range(ADIM):
                index = jnp.where(row_at == f * SLOTS + first + a, teacher_ref[f, a], index)
        return (index == bin_at).astype(F32)

    def action_stream():
        loads[2].wait()
        looked = jnp.dot(one_hot(1).astype(BF16), table[...], preferred_element_type=F32)
        slot = lax.broadcasted_iota(jnp.int32, looked.shape, 0) % SLOTS
        act[...] = jnp.where(slot == 0, rows_ref[1:2, :].astype(F32), looked)
        rows_f = act[...]
        scale = lax.rsqrt(jnp.mean(rows_f * rows_f, axis=-1, keepdims=True) + eps)
        nact[...] = (rows_f * scale * rows_ref[0:1, :].astype(F32)).astype(BF16)
        nact_all[place] = nact[:, pl.ds(aligned(me * depth, depth), depth)]
        for m in range(1, 8):
            act_send(m).start()

    tile = 512

    def action_partial():
        for m in range(1, 8):
            act_send(m).wait_recv()
        stacked = nact_all[...].reshape(8 * slots, depth)

        def act_tile(j, carry):
            at = pl.ds(aligned(j * tile, tile), tile)
            value = jnp.dot(stacked, w_ref[:, at], preferred_element_type=F32).astype(BF16)
            apart[:, :, at] = value.reshape(8, slots, tile)
            return carry

        lax.fori_loop(0, wide // tile, act_tile, 0)
        apart_c().start()

    def action_sum_1():
        apart_c().wait_recv()
        for one in range(2):
            for two in range(2):
                at = (1 - c) * (2 * one + two) + c * (2 * two + one)
                value = apart[c * 4 + at].astype(F32) + apart_in_c[at].astype(F32)
                apart_two[2 * one + two] = value.astype(BF16)
        apart_1().start()

    def action_sum_2():
        apart_1().wait_recv()
        for two in range(2):
            value = apart_two[2 * b1 + two].astype(F32) + apart_in_1[two].astype(F32)
            apart_one[two] = value.astype(BF16)
        apart_2().start()

    gain_own = rows_ref[0:1, pl.ds(aligned(me * depth, depth), depth)].astype(F32)

    def spread_done(i):
        for p in range(pairs):
            home = pairs * y + p

            @pl.when((z >= home) & (z < n_t - 1))
            def _():
                z_right(p, i, False).wait_send()

            @pl.when((z <= home) & (z > 0))
            def _():
                z_left(p, i, False).wait_send()

    off_c = c * half
    off_1 = off_c + b1 * fourth
    off_2 = off_1 + b2 * eighth

    def at_c(i):
        return remote(send_c.at[i % 2], recv_c.at[i], c_s.at[i], c_r.at[i], dev_c)

    def at_1(i):
        return remote(send_1.at[i % 2], recv_1.at[i], s1_s.at[i], s1_r.at[i], dev_1)

    def at_2(i):
        return remote(send_2.at[i % 2], recv_2.at[i], s2_s.at[i], s2_r.at[i], dev_2)

    def back_2(i):
        block = merged.at[rows_of(i), pl.ds(aligned(off_2), eighth)]
        return remote(block, block, g2_s.at[i], g2_r.at[i], dev_2)

    def back_1(i):
        block = merged.at[rows_of(i), pl.ds(aligned(off_1), fourth)]
        return remote(block, block, g1_s.at[i], g1_r.at[i], dev_1)

    def back_c(i):
        block = merged.at[rows_of(i), pl.ds(aligned(off_c), half)]
        return remote(block, block, gc_s.at[i], gc_r.at[i], dev_c)

    def stage_c(i):
        @pl.when(i >= 2)
        def _():
            at_c(i - 2).wait_send()

        block = jnp.concatenate([pair[p, rows_of(i)] for p in range(pairs)], axis=1)
        block = (block.astype(F32) * gain_own).astype(BF16)

        def away(j, carry):
            at = pl.ds(aligned((1 - c) * half + j * tile), tile)
            value = jnp.dot(block, w_ref[:, at], preferred_element_type=F32)
            send_c[i % 2, :, pl.ds(aligned(j * tile, tile), tile)] = value.astype(BF16)
            return carry

        lax.fori_loop(0, half // tile, away, 0)
        at_c(i).start()

        def kept(j, carry):
            at = pl.ds(aligned(c * half + j * tile), tile)
            own_c[i % 2, :, pl.ds(aligned(j * tile, tile), tile)] = jnp.dot(block, w_ref[:, at], preferred_element_type=F32)
            return carry

        lax.fori_loop(0, half // tile, kept, 0)

    def stage_1(i):
        @pl.when(i >= 2)
        def _():
            at_1(i - 2).wait_send()

        at_c(i).wait_recv()
        away = pl.ds(aligned((1 - b1) * fourth), fourth)
        send_1[i % 2] = (own_c[i % 2, :, away] + recv_c[i, :, away].astype(F32)).astype(BF16)
        at_1(i).start()
        kept = pl.ds(aligned(b1 * fourth), fourth)
        own_1[...] = own_c[i % 2, :, kept] + recv_c[i, :, kept].astype(F32)

    def stage_2(i):
        @pl.when(i >= 2)
        def _():
            at_2(i - 2).wait_send()

        at_1(i).wait_recv()
        away = pl.ds(aligned((1 - b2) * eighth), eighth)
        send_2[i % 2] = (own_1[:, away] + recv_1[i, :, away].astype(F32)).astype(BF16)
        at_2(i).start()
        kept = pl.ds(aligned(b2 * eighth), eighth)
        own_2[...] = own_1[:, kept] + recv_1[i, :, kept].astype(F32)

    def stage_3(i):
        at_2(i).wait_recv()
        merged[rows_of(i), pl.ds(aligned(off_2), eighth)] = (own_2[...] + recv_2[i].astype(F32)).astype(BF16)
        back_2(i).start()

    def stage_4(i):
        back_2(i).wait_recv()
        back_1(i).start()

    def stage_5(i):
        back_1(i).wait_recv()
        back_c(i).start()

    def gather_add(first, count):
        for i in range(count):
            back_c(first + i).wait_recv()
        deep = pl.ds(aligned(first * ROWS, ROWS), count * ROWS)
        left = patch[:, :, deep].reshape(n_t * rows, count * ROWS)

        def one(j, carry):
            at = pl.ds(aligned(j * tile, tile), tile)
            value = jnp.dot(left, merged[deep, at], preferred_element_type=F32)

            @pl.when(first == 0)
            def _():
                total[:, at] = value

            @pl.when(first > 0)
            def _():
                total[:, at] += value

            return carry

        lax.fori_loop(0, wide // tile, one, 0)

    def square_send(k):
        to = (z + k) % n_t
        return remote(squares.at[to], squares_in.at[z], sq_s.at[k - 1], sq_r.at[k - 1], (dp, to, y))

    def factor_send(k):
        return remote(factor, factor_in.at[z], fa_s.at[k - 1], fa_r.at[k - 1], (dp, (z + k) % n_t, y))

    def embed():
        for t in range(n_t):
            lanes = jnp.zeros((rows, 128), F32)
            for d in range(quarter.shape[0]):
                value = jnp.dot(patch[t], quarter[d], preferred_element_type=F32).astype(BF16)
                emb[t, :, d * duo : (d + 1) * duo] = value
                value = value.astype(F32)
                value = value * value
                for e in range(duo // 128):
                    lanes = lanes + value[:, e * 128 : (e + 1) * 128]
            squares[t] = lanes
        squares_in[z] = squares[z]
        for k in range(1, n_t):
            square_send(k).start()

    def row_factor():
        for k in range(1, n_t):
            square_send(k).wait_recv()
        lanes = squares_in[0]
        for t in range(1, n_t):
            lanes = lanes + squares_in[t]
        mean = jnp.sum(lanes, axis=-1, keepdims=True) * (1.0 / D)
        factor[...] = jnp.broadcast_to(lax.rsqrt(mean + eps), factor.shape)
        factor_in[z] = factor[...]
        for k in range(1, n_t):
            factor_send(k).start()

    def own_action_rows():
        apart_2().wait_recv()
        qkv_act[...] = (apart_one[b2].astype(F32) + apart_in_2[...].astype(F32)).astype(BF16)

    me_1 = dev_1[0] * 2 + dev_1[2]
    me_2 = dev_2[0] * 2 + dev_2[2]
    me_12 = dp_x * 2 + y_n
    lineage = (me, me_1, me_2, me_12)

    def wo_core(k):
        block = wo_ref.at[lineage[k]]
        return remote(block, block, wo_s.at[k], wo_r.at[k], dev_c)

    pieces = 8
    piece = width // pieces

    def wo_first(i):
        block = wo_ref.at[me, pl.ds(i * piece, piece)]
        return remote(block, block, wf_s.at[i], wf_r.at[i], dev_1)

    def wo_second(k):
        block = wo_ref.at[lineage[k]]
        return remote(block, block, wo_s.at[5 + k], wo_r.at[5 + k], dev_2)

    ahead = 3
    first_pair()
    proj_y(1).wait_recv()
    own_pair(1)
    first_spread()
    proj_y(2).wait_recv()
    own_pair(2)
    spread(1)
    loads[1].wait()
    for k in (3, 4, 5):
        loads[k].wait()

    def step(s, carry):
        @pl.when(s == 0)
        def _():
            proj_y(ahead).wait_recv()

        @pl.when(s == 1)
        def _():
            for i in range(ahead + 1, chunks):
                proj_y(i).wait_recv()
            proj_x().wait_recv()
            proj_diag().start()
            proj_core(0).start()

        @pl.when(s + ahead < chunks)
        def _():
            own_pair(s + ahead)

        @pl.when((s >= 5) & (s < chunks + 5))
        def _():
            stage_5(s - 5)

        @pl.when((s >= 4) & (s < chunks + 4))
        def _():
            stage_4(s - 4)

        @pl.when((s >= 3) & (s < chunks + 3))
        def _():
            stage_3(s - 3)

        @pl.when((s >= 2) & (s < chunks + 2))
        def _():
            stage_2(s - 2)

        @pl.when((s >= 1) & (s < chunks + 1))
        def _():
            stage_1(s - 1)

        @pl.when(s + 2 < chunks)
        def _():
            spread(s + 2)

        @pl.when(s < chunks)
        def _():
            stage_c(s)

        @pl.when((s >= 1) & (s <= 3))
        def _():
            for k in range(1, n_t):
                patch_send(k, s - 1).start()

        for i in range(3, chunks):
            @pl.when(s == 4 + (i - 3) // 2)
            def _():
                for k in range(1, n_t):
                    patch_send(k, i).start()

        @pl.when((s >= 4) & (s <= chunks))
        def _():
            for k in range(1, n_t):
                patch_send(k, s - 4).wait_recv()

        @pl.when(s == chunks + 1)
        def _():
            for i in range(chunks - 3, chunks):
                for k in range(1, n_t):
                    patch_send(k, i).wait_recv()

        @pl.when((s >= 7) & (s % 2 == 1) & (s < chunks + 5))
        def _():
            gather_add(s - 7, 2)

        @pl.when(s == 1)
        def _():
            action_stream()

        @pl.when(s == 3)
        def _():
            action_partial()

        @pl.when(s == chunks - 1)
        def _():
            action_sum_1()

        @pl.when(s == chunks + 1)
        def _():
            action_sum_2()

        @pl.when(s == chunks - ahead + 1)
        def _():
            proj_diag().wait_recv()
            proj_core(1).start()
            loads[6].wait()
            wo_core(0).start()

        @pl.when(s == chunks)
        def _():
            proj_core(0).wait_recv()
            proj_core(1).wait_recv()

        @pl.when(s == chunks + 1)
        def _():
            embed()

        @pl.when(s == chunks + 3)
        def _():
            row_factor()

        for i in range(3):
            @pl.when(s == chunks + i)
            def _():
                wo_first(i).start()

        @pl.when(s == chunks + 3)
        def _():
            for i in range(3, pieces):
                wo_first(i).start()

        return carry

    lax.fori_loop(0, chunks + 5, step, 0)
    if chunks % 2:
        gather_add(chunks - 1, 1)

    for k in range(1, n_t):
        factor_send(k).wait_recv()

    def scale_tile(j, carry):
        at = pl.ds(aligned(j * tile, tile), tile)
        for t in range(n_t):
            for f in range(frames):
                piece = pl.ds(t * rows + f * local, local)
                value = total[piece, at] * factor_in[t, f * local : (f + 1) * local, 0:1]
                qkv[f, t * local : (t + 1) * local, at] = value.astype(BF16)
        return carry

    lax.fori_loop(0, wide // tile, scale_tile, 0)

    inv_root = 1.0 / math.sqrt(HD)
    length = n_t * local
    nt = (((1,), (1,)), ((), ()))
    block = length // 2
    causal = [
        lax.broadcasted_iota(jnp.int32, (block, (u + 1) * block), 0) + u * block
        >= lax.broadcasted_iota(jnp.int32, (block, (u + 1) * block), 1)
        for u in range(2)
    ]
    slot_i = lax.broadcasted_iota(jnp.int32, (slots, slots), 0)
    slot_j = lax.broadcasted_iota(jnp.int32, (slots, slots), 1)
    slot_sees = (slot_i // SLOTS == slot_j // SLOTS) & (slot_i >= slot_j)
    slot_frame = lax.broadcasted_iota(jnp.int32, (slots, HD), 0) // SLOTS

    def patch_heads(h, carry):
        qc, kc, vc = (pl.ds(aligned(part_at * width + h * HD), HD) for part_at in range(3))
        units = [(f, u) for f in range(frames) for u in range(2)]
        scores = [
            lax.dot_general(
                qkv[f, u * block : (u + 1) * block, qc],
                qkv[f, : (u + 1) * block, kc],
                nt,
                preferred_element_type=F32,
            )
            for f, u in units
        ]
        scores = [jnp.where(causal[u], one * inv_root, -1e30) for one, (f, u) in zip(scores, units)]
        scores = [jnp.exp(one - jnp.max(one, axis=-1, keepdims=True)) for one in scores]
        scores = [(one * (1.0 / jnp.sum(one, axis=-1, keepdims=True))).astype(BF16) for one in scores]
        for one, (f, u) in zip(scores, units):
            value = jnp.dot(one, qkv[f, : (u + 1) * block, vc], preferred_element_type=F32).astype(BF16)
            for t in range(n_t // 2):
                mixed[u * (n_t // 2) + t, f * local : (f + 1) * local, pl.ds(aligned(h * HD), HD)] = value[
                    t * local : (t + 1) * local
                ]
        return carry

    lax.fori_loop(0, heads, patch_heads, 0, unroll=2)

    def action_heads():
        for h in range(heads):
            qc, kc, vc = (pl.ds(part_at * width + h * HD, HD) for part_at in range(3))
            qa, ka, va = qkv_act[:, qc], qkv_act[:, kc], qkv_act[:, vc]
            near = lax.dot_general(qa, ka, nt, preferred_element_type=F32) * inv_root
            near = jnp.where(slot_sees, near, -1e30)
            mixed_slots = jnp.zeros((slots, HD), F32)
            for f in range(frames):
                k, v = qkv[f, :, kc], qkv[f, :, vc]
                far = lax.dot_general(qa, k, nt, preferred_element_type=F32) * inv_root
                top = jnp.maximum(jnp.max(far, axis=-1, keepdims=True), jnp.max(near, axis=-1, keepdims=True))
                far, close = jnp.exp(far - top), jnp.exp(near - top)
                below = 1.0 / (jnp.sum(far, axis=-1, keepdims=True) + jnp.sum(close, axis=-1, keepdims=True))
                value = jnp.dot((far * below).astype(BF16), v, preferred_element_type=F32)
                value = value + jnp.dot((close * below).astype(BF16), va, preferred_element_type=F32)
                mixed_slots = jnp.where(slot_frame == f, value, mixed_slots)
            mixed_act[:, h * HD : (h + 1) * HD] = mixed_slots.astype(BF16)

    def block_of(j, e):
        xs, ys = ((x, y), (x, y), (1 - x, y), (x, 1 - y), (x, 1 - y), (1 - x, y), (1 - x, 1 - y), (1 - x, 1 - y))[
            2 * j + e
        ]
        return 4 * xs + 2 * e + ys

    def contribution(t, j):
        left = mixed[t]
        for e in range(2):
            g = block_of(j, e)
            part[:, e * depth : (e + 1) * depth] = jnp.dot(left, wo_ref[g], preferred_element_type=F32)

            @pl.when(z // pairs == g % 2)
            def _():
                at = pl.ds(aligned(e * depth + (z % pairs) * duo), duo)
                part[:, at] += emb[t, :, pl.ds(aligned((g // 2) * duo), duo)].astype(F32)

    line = n_t - 1

    def to_right(n):
        return remote(right_out.at[n], right_in.at[n], rr_s.at[n], rr_r.at[n], (dp, lax.rem(z + 1, n_t), y))

    def to_left(n):
        return remote(left_out.at[n], left_in.at[n], rl_s.at[n], rl_r.at[n], (dp, lax.rem(z + n_t - 1, n_t), y))

    def go_right(j, m):
        n = j * line + m
        contribution(line - m, j)

        @pl.when(z > 0)
        def _():
            to_right(n).wait_recv()
            part[...] += right_in[n].astype(F32)

        right_out[n] = part[...].astype(BF16)
        to_right(n).start()

    def go_left(j, m):
        n = j * line + m
        contribution(m, j)

        @pl.when(z < line)
        def _():
            to_left(n).wait_recv()
            part[...] += left_in[n].astype(F32)

        left_out[n] = part[...].astype(BF16)
        to_left(n).start()

    def aup_send(j):
        return remote(aup.at[j], aup_in.at[z], au_s.at[j], au_r.at[z], (dp, j, y))

    def put(j, e):
        at = pl.ds(aligned(block_of(j, e) * depth, depth), depth)
        return pltpu.make_async_copy(stage.at[:, at], out_hbm.at[:, at], local_sem.at[10 + 2 * j + e])

    def finish(j):
        contribution(z, j)

        @pl.when(z > 0)
        def _():
            n = j * line + line - z
            to_right(n).wait_recv()
            part[...] += right_in[n].astype(F32)

        @pl.when(z < n_t - 1)
        def _():
            n = j * line + z
            to_left(n).wait_recv()
            part[...] += left_in[n].astype(F32)

        for e in range(2):
            at = pl.ds(aligned(block_of(j, e) * depth, depth), depth)
            stage[:, at] = part[:, e * depth : (e + 1) * depth].astype(BF16)
            put(j, e).start()

    def asq_send(k):
        return remote(asq, asq_in.at[z], aq_s.at[k - 1], aq_r.at[k - 1], (dp, (z + k) % n_t, y))

    def alog_send(k):
        return remote(alog, alog_in.at[z], al_s.at[k - 1], al_r.at[k - 1], (dp, (z + k) % n_t, y))

    def head_load(j, e):
        at = pl.ds(aligned(block_of(j, e) * depth, depth), depth)
        return pltpu.make_async_copy(head_hbm.at[at], head.at[pl.ds(e * depth, depth)], local_sem.at[7 + e])

    def action_update():
        for j in range(4):
            for e in range(2):
                aup[j, :, e * depth : (e + 1) * depth] = jnp.dot(
                    mixed_act[...], wo_ref[block_of(j, e)], preferred_element_type=F32
                ).astype(BF16)

            @pl.when(z != j)
            def _():
                aup_send(j).start()

            @pl.when(z == j)
            def _():
                for e in range(2):
                    head_load(j, e).start()

    def action_norm():
        for j in range(4):
            @pl.when(z == j)
            def _():
                aup_in[j] = aup[j]
                for t in range(n_t):
                    if t != j:
                        remote(aup.at[j], aup_in.at[t], au_s.at[j], au_r.at[t], (dp, j, y)).wait_recv()
                value = aup_in[0].astype(F32)
                for t in range(1, n_t):
                    value = value + aup_in[t].astype(F32)
                lanes = jnp.zeros((slots, 128), F32)
                for e in range(2):
                    at = pl.ds(aligned(block_of(j, e) * depth, depth), depth)
                    acted_e = value[:, e * depth : (e + 1) * depth] + act[:, at]
                    acted[0, :, e * depth : (e + 1) * depth] = acted_e
                    acted[1, :, e * depth : (e + 1) * depth] = jnp.broadcast_to(
                        rows_ref[2:3, at].astype(F32), (slots, depth)
                    )
                    for q in range(depth // 128):
                        piece = acted_e[:, q * 128 : (q + 1) * 128]
                        lanes = lanes + piece * piece
                asq[...] = lanes

        asq_in[z] = asq[...]
        for k in range(1, n_t):
            asq_send(k).start()

    def action_logits():
        for e in range(2):
            head_load(0, e).wait()
        for k in range(1, n_t):
            asq_send(k).wait_recv()
        lanes = asq_in[0]
        for t in range(1, n_t):
            lanes = lanes + asq_in[t]
        scale = lax.rsqrt(jnp.sum(lanes, axis=-1, keepdims=True) * (1.0 / D) + eps)
        final = (acted[0] * scale * acted[1]).astype(BF16)
        alog[...] = jnp.dot(final, head[...], preferred_element_type=F32)
        alog_in[z] = alog[...]
        for k in range(1, n_t):
            alog_send(k).start()

    def action_loss():
        for k in range(1, n_t):
            alog_send(k).wait_recv()
        logits = alog_in[0]
        for t in range(1, n_t):
            logits = logits + alog_in[t]
        picked = jnp.sum(logits * one_hot(0), axis=-1, keepdims=True)
        top = jnp.max(logits, axis=-1, keepdims=True)
        spread_out = jnp.log(jnp.sum(jnp.exp(logits - top), axis=-1, keepdims=True)) + top
        at_lane = lax.broadcasted_iota(jnp.int32, (slots, 128), 1) == lax.broadcasted_iota(
            jnp.int32, (slots, 128), 0
        ) % SLOTS
        lanes = jnp.where(at_lane, spread_out - picked, 0.0)
        loss_ref[...] = jnp.sum(lanes.reshape(frames, SLOTS, 128), axis=1)[:, :ADIM]

    def drained():
        for i in range(chunks):
            proj_y(i).wait_send()
            back_2(i).wait_send()
            back_1(i).wait_send()
            back_c(i).wait_send()
            if i > 0:
                spread_done(i)
        for i in range(chunks - 2, chunks):
            at_c(i).wait_send()
            at_1(i).wait_send()
            at_2(i).wait_send()
        for copy in (apart_c(), apart_1(), apart_2()):
            copy.wait_send()
        for p in range(pairs):
            @pl.when(z == pairs * y + p)
            def _():
                for k in range(1, n_t):
                    z_first(p, k).wait_send()

        proj_x().wait_send()
        proj_diag().wait_send()
        for k in range(2):
            proj_core(k).wait_send()
        for m in range(1, 8):
            act_send(m).wait_send()
        for k in range(1, n_t):
            for i in range(chunks):
                patch_send(k, i).wait_send()
            square_send(k).wait_send()
            factor_send(k).wait_send()

    for j in range(4):
        if j == 0:
            wo_core(0).wait_recv()
        elif j == 1:
            own_action_rows()
            action_heads()
            wo_core(1).wait_recv()
        elif j == 2:
            wo_second(0).wait_recv()
            wo_core(2).start()
            wo_second(1).wait_recv()
            wo_core(3).start()
            wo_core(2).wait_recv()
            wo_core(3).wait_recv()
            action_update()
        else:
            action_norm()

        def shift(m, carry):
            t = line - m

            near_right = z < n_t // 2

            @pl.when(near_right & (z < t))
            def _():
                go_right(j, m)

            @pl.when((z >= n_t // 2) & (z > m))
            def _():
                go_left(j, m)

            @pl.when((m >= 1) & (z >= n_t // 2) & (z < t + 1))
            def _():
                go_right(j, m - 1)

            @pl.when((m >= 1) & near_right & (z > m - 1))
            def _():
                go_left(j, m - 1)

            return carry

        shift(0, 0)
        if j == 0:
            for i in range(pieces):
                wo_first(i).wait_recv()
            wo_core(1).start()
            wo_second(0).start()
            wo_second(1).start()
        elif j == 3:
            action_logits()
        lax.fori_loop(1, line, shift, 0)
        if 0 < j < 3:
            finish(j - 1)
        if j == 1:
            drained()

    finish(2)
    action_loss()
    finish(3)

    for j in range(4):
        for e in range(2):
            put(j, e).wait()
    for k in range(1, n_t):
        asq_send(k).wait_send()
        alog_send(k).wait_send()
    for k in range(4):
        wo_core(k).wait_send()
    for i in range(pieces):
        wo_first(i).wait_send()
    wo_second(0).wait_send()
    wo_second(1).wait_send()
    for n in range(4 * line):
        @pl.when(z < line - n % line)
        def _():
            to_right(n).wait_send()

        @pl.when(z > n % line)
        def _():
            to_left(n).wait_send()
    for j in range(4):
        @pl.when(z != j)
        def _():
            aup_send(j).wait_send()


def fits(mesh, patches, proj_w, wq, wo):
    frames, local, vision = patches.shape
    n_t = mesh.shape["tensor"]
    return (
        mesh.shape["dp"] == 4
        and mesh.shape["section"] == 2
        and n_t == 4
        and proj_w.shape[1] % 128 == 0
        and 8 * wq.shape[0] == D
        and n_t * wq.shape[1] == D
        and vision % (3 * ROWS) == 0
        and local % 16 == 0
        and frames * SLOTS % 16 == 0
    )


def program(
    mesh, patches, teacher, proj_w, norm_gain, wq, wk, wv, wo, start_row, action_table, final_gain, head_w
):
    if not fits(mesh, patches, proj_w, wq, wo):
        return on_device(
            patches, teacher, proj_w, norm_gain, wq, wk, wv, wo, start_row, action_table, final_gain, head_w
        )
    frames, local, vision = patches.shape
    n_t = mesh.shape["tensor"]
    rows, slots = frames * local, frames * SLOTS
    depth, width = wq.shape
    cols = proj_w.shape[1]
    wide, chunks, pairs, line = 3 * width, vision // ROWS, n_t // 2, n_t - 1
    vmem, anywhere = pl.BlockSpec(memory_space=pltpu.VMEM), pl.BlockSpec(memory_space=pl.ANY)
    dma = pltpu.SemaphoreType.DMA
    scratch = [
        pltpu.VMEM((3, D), BF16),
        pltpu.VMEM((depth, wide), BF16),
        pltpu.VMEM((8,) + wo.shape, BF16),
        pltpu.VMEM((4, vision, 2 * cols), BF16),
        pltpu.VMEM((pairs, vision, 2 * cols), BF16),
        pltpu.VMEM((n_t, rows, vision), BF16),
        pltpu.VMEM(action_table.shape, BF16),
        pltpu.VMEM((2 * depth, BINS), BF16),
        pltpu.VMEM((2, ROWS, wide // 2), BF16),
        pltpu.VMEM((chunks, ROWS, wide // 2), BF16),
        pltpu.VMEM((2, ROWS, wide // 4), BF16),
        pltpu.VMEM((chunks, ROWS, wide // 4), BF16),
        pltpu.VMEM((2, ROWS, wide // 8), BF16),
        pltpu.VMEM((chunks, ROWS, wide // 8), BF16),
        pltpu.VMEM((2, ROWS, wide // 2), F32),
        pltpu.VMEM((ROWS, wide // 4), F32),
        pltpu.VMEM((ROWS, wide // 8), F32),
        pltpu.VMEM((vision, wide), BF16),
        pltpu.VMEM((n_t * rows, wide), F32),
        pltpu.VMEM((frames, n_t * local, wide), BF16),
        pltpu.VMEM((n_t, rows, width), BF16),
        pltpu.VMEM((n_t, rows, 8 * cols), BF16),
        pltpu.VMEM((n_t, rows, 128), F32),
        pltpu.VMEM((n_t, rows, 128), F32),
        pltpu.VMEM((rows, 128), F32),
        pltpu.VMEM((n_t, rows, 128), F32),
        pltpu.VMEM((slots, D), F32),
        pltpu.VMEM((slots, D), BF16),
        pltpu.VMEM((8, slots, depth), BF16),
        pltpu.VMEM((8, slots, wide), BF16),
        pltpu.VMEM((4, slots, wide), BF16),
        pltpu.VMEM((4, slots, wide), BF16),
        pltpu.VMEM((2, slots, wide), BF16),
        pltpu.VMEM((2, slots, wide), BF16),
        pltpu.VMEM((slots, wide), BF16),
        pltpu.VMEM((slots, wide), BF16),
        pltpu.VMEM((slots, width), BF16),
        pltpu.VMEM((n_t, slots, 2 * depth), BF16),
        pltpu.VMEM((n_t, slots, 2 * depth), BF16),
        pltpu.VMEM((slots, 128), F32),
        pltpu.VMEM((n_t, slots, 128), F32),
        pltpu.VMEM((slots, BINS), F32),
        pltpu.VMEM((n_t, slots, BINS), F32),
        pltpu.VMEM((rows, D), BF16),
        pltpu.VMEM((2, slots, 2 * depth), F32),
        pltpu.VMEM((4 * line, rows, 2 * depth), BF16),
        pltpu.VMEM((4 * line, rows, 2 * depth), BF16),
        pltpu.VMEM((4 * line, rows, 2 * depth), BF16),
        pltpu.VMEM((4 * line, rows, 2 * depth), BF16),
        pltpu.VMEM((rows, 2 * depth), F32),
        dma((18,)),
        dma((chunks,)), dma((chunks,)),
        dma, dma, dma, dma,
        dma((2,)), dma((2,)),
        dma((pairs, chunks)), dma((pairs, chunks)), dma((pairs, chunks)), dma((line,)),
        dma((line, chunks)), dma((line, chunks)),
        dma((7,)), dma((7,)), dma((3,)), dma((3,)),
    ]
    scratch += [dma((chunks,))] * 12
    scratch += [dma((line,))] * 4
    scratch += [dma((7,))] * 2 + [dma((8,))] * 2
    scratch += [dma((4 * line,))] * 4
    scratch += [dma((n_t,))] * 2 + [dma((line,))] * 4
    hidden, loss = pl.pallas_call(
        functools.partial(fused, (n_t, frames, local)),
        out_shape=(
            jax.ShapeDtypeStruct((rows, D), BF16),
            jax.ShapeDtypeStruct((frames, ADIM), F32),
        ),
        in_specs=[pl.BlockSpec(memory_space=pltpu.SMEM)] + [anywhere] * 9,
        out_specs=(anywhere, vmem),
        scratch_shapes=scratch,
        compiler_params=pltpu.CompilerParams(
            collective_id=0, has_side_effects=True, vmem_limit_bytes=67043328
        ),
    )(
        teacher,
        jnp.stack([norm_gain, start_row, final_gain]),
        patches.reshape(rows, vision),
        proj_w,
        wq,
        wk,
        wv,
        wo,
        action_table,
        head_w,
    )
    return hidden.reshape(frames, local, D), loss


def solution(mesh):
    return jax.shard_map(
        functools.partial(program, mesh),
        mesh=mesh,
        in_specs=(
            P(("dp", "section"), "tensor", None),
            P(("dp", "section"), None),
            P(None, ("dp", "tensor", "section")),
            P(),
            P(("dp", "section"), "tensor"),
            P(("dp", "section"), "tensor"),
            P(("dp", "section"), "tensor"),
            P("tensor", ("dp", "section")),
            P(),
            P(),
            P(),
            P(),
        ),
        out_specs=(P(("dp", "section"), "tensor", None), P(("dp", "section"), None)),
        check_vma=False,
    )
```

```python
import functools
import math

import jax
import jax.numpy as jnp
from jax import lax
from jax.experimental import pallas as pl
from jax.experimental.pallas import tpu as pltpu
from jax.sharding import PartitionSpec as P

D = 4096
HD = 128
V = 1152
P_SIZE = 256
BINS = 256
ADIM = 7
SLOTS = 8


eps = 1e-05


def normalize(rows, gain):
    rows = rows.astype(jnp.float32)
    factor = lax.rsqrt(jnp.mean(rows * rows, axis=-1, keepdims=True) + eps)
    return rows * factor * gain.astype(jnp.float32)


def action_rows(teacher, start_row, action_table):
    frames = teacher.shape[0]
    onehot = (teacher[..., None] == jnp.arange(BINS, dtype=jnp.int32)).astype(jnp.bfloat16)
    looked = jnp.dot(onehot.reshape(-1, BINS), action_table, preferred_element_type=jnp.float32)
    looked = looked.astype(jnp.bfloat16).reshape(frames, ADIM, D)
    start = jnp.broadcast_to(start_row.reshape(1, 1, D), (frames, 1, D))
    return jnp.concatenate([start, looked], axis=1)


def line_gather(own, axis):
    n = lax.axis_size(axis)
    here = lax.axis_index(axis)
    right = left = own
    from_left, from_right = [], []
    for r in range(n - 1):
        right = lax.ppermute(right, axis, [(t, t + 1) for t in range(r, n - 1)])
        left = lax.ppermute(left, axis, [(t, t - 1) for t in range(1, n - r)])
        from_left.append(right)
        from_right.append(left)
    blocks = jnp.zeros((n,) + own.shape, own.dtype)
    blocks = lax.dynamic_update_index_in_dim(blocks, own, here, 0)
    for r in range(n - 1):
        block = jnp.where(here > r, from_left[r], from_right[n - 2 - r])
        blocks = lax.dynamic_update_index_in_dim(blocks, block, lax.rem(here - 1 - r + n, n), 0)
    return blocks


def line_reduce_scatter(parts, axis):
    n = lax.axis_size(axis)
    here = lax.axis_index(axis)

    def part(c):
        return lax.dynamic_index_in_dim(parts, jnp.clip(c, 0, n - 1), 0, keepdims=False)

    right = left = None
    for r in range(n - 1):
        steps = range(min(r, n - 2) + 1)
        to_right = part(n - 1 - r + here)
        to_left = part(r - (n - 1) + here)
        if right is not None:
            to_right = to_right + right.astype(jnp.float32)
            to_left = to_left + left.astype(jnp.float32)
        right = lax.ppermute(to_right.astype(jnp.bfloat16), axis, [(t, t + 1) for t in steps])
        left = lax.ppermute(
            to_left.astype(jnp.bfloat16), axis, [(n - 1 - t, n - 2 - t) for t in steps]
        )
    total = part(here)
    if right is not None:
        total = total + right.astype(jnp.float32) + left.astype(jnp.float32)
    return total


def plane_columns(own):
    rows, columns = own.shape
    blocks = line_gather(line_gather(own, "section").reshape(-1, columns), "dp")
    blocks = blocks.reshape(-1, rows, columns)
    return jnp.concatenate([blocks[i] for i in range(blocks.shape[0])], axis=1)


RELAYS = 2


def on_device(
    patches, teacher, proj_w, norm_gain, wq, wk, wv, wo, start_row, action_table, final_gain, head_w
):
    frames = patches.shape[0]
    local_patches = patches.shape[1]
    length = P_SIZE + SLOTS
    plane = ("dp", "section")
    n_dp, n_t = lax.axis_size("dp"), lax.axis_size("tensor")
    here = lax.axis_index("tensor")
    proj_part = plane_columns(proj_w)
    all_patches = line_gather(patches.reshape(-1, V), "tensor")
    all_patches = all_patches.reshape(n_t, frames, local_patches, V).transpose(1, 0, 2, 3)
    embedded_part = jnp.dot(
        all_patches.reshape(-1, V), proj_part, preferred_element_type=jnp.float32
    ).astype(jnp.bfloat16)
    blocks = line_gather(embedded_part, "tensor")
    width = embedded_part.shape[1] // n_dp
    embedded_all = jnp.concatenate(
        [blocks[t, :, d * width : (d + 1) * width] for d in range(n_dp) for t in range(n_t)], axis=1
    ).reshape(frames, P_SIZE, D)
    embedded_own = lax.dynamic_slice_in_dim(embedded_all, here * local_patches, local_patches, 1)
    actions = action_rows(teacher, start_row, action_table)
    stream = jnp.concatenate([embedded_all, actions], axis=1)
    normed = normalize(stream, norm_gain).astype(jnp.bfloat16).reshape(-1, D)
    full_out = plane_columns(wo)
    local_width = wq.shape[1]
    projected = tuple(
        jnp.dot(
            normed,
            lax.all_gather(weight, plane, axis=0, tiled=True),
            preferred_element_type=jnp.float32,
        )
        for weight in (wq, wk, wv)
    )
    heads_local = local_width // HD
    queries, keys_all, values_all = [
        part.astype(jnp.bfloat16).reshape(frames, length, heads_local, HD) for part in projected
    ]
    inv_root = 1.0 / math.sqrt(HD)
    scores = (
        jnp.einsum("fqhd,fkhd->fhqk", queries, keys_all, preferred_element_type=jnp.float32)
        * inv_root
    )
    positions = jnp.arange(length, dtype=jnp.int32)
    causal = positions[:, None] >= positions[None, :]
    scores = jnp.where(causal[None, None], scores, -1e30)
    weights = jax.nn.softmax(scores, axis=-1).astype(jnp.bfloat16)
    mixed = jnp.einsum("fhqk,fkhd->fqhd", weights, values_all, preferred_element_type=jnp.float32)
    mixed = mixed.astype(jnp.bfloat16).reshape(frames, length, local_width)
    patch_rows = mixed[:, :P_SIZE].reshape(frames, n_t, local_patches, local_width)
    patch_rows = patch_rows.transpose(1, 0, 2, 3).reshape(n_t, -1, local_width)
    slot_rows = mixed[:, P_SIZE:].reshape(-1, local_width)
    slot_part = jnp.dot(slot_rows, full_out, preferred_element_type=jnp.float32)
    slot_parts = line_gather(slot_part.astype(jnp.bfloat16), "tensor")
    slot_update = jnp.sum(slot_parts.astype(jnp.float32), axis=0)
    chunk = D // RELAYS
    updates = []
    for j in range(RELAYS):
        parts = jnp.einsum(
            "nrw,wc->nrc",
            patch_rows,
            full_out[:, j * chunk : (j + 1) * chunk],
            preferred_element_type=jnp.float32,
        )
        updates.append(line_reduce_scatter(parts, "tensor"))
    update = jnp.concatenate(updates, axis=1).reshape(frames, local_patches, D)
    hidden_out = (embedded_own.astype(jnp.float32) + update).astype(jnp.bfloat16)
    acted = (actions.astype(jnp.float32) + slot_update.reshape(frames, SLOTS, D))[:, :ADIM]
    final = normalize(acted, final_gain).astype(jnp.bfloat16).reshape(-1, D)
    logits = jnp.dot(final, head_w, preferred_element_type=jnp.float32).reshape(frames, ADIM, BINS)
    chosen = (teacher[..., None] == jnp.arange(BINS, dtype=jnp.int32)).astype(jnp.float32)
    picked = jnp.sum(logits * chosen, axis=-1)
    loss = jax.nn.logsumexp(logits, axis=-1) - picked
    return (hidden_out, loss)


MESH = pl.DeviceIdType.MESH
ROWS = 128
F32 = jnp.float32
BF16 = jnp.bfloat16


def aligned(value, to=128):
    return pl.multiple_of(value, to)


def fused(
    sizes,
    teacher_ref, rows_hbm,
    patches_hbm, proj_hbm, wq_hbm, wk_hbm, wv_hbm, wo_hbm, table_hbm, head_hbm,
    out_hbm, loss_ref,
    rows_ref, w_ref, wo_ref, quarter, pair, patch, table, head,
    send_c, recv_c, send_1, recv_1, send_2, recv_2, own_c, own_1, own_2, merged,
    total, qkv, mixed, emb, squares, squares_in, factor, factor_in,
    act, nact, nact_all, apart, apart_in_c, apart_two, apart_in_1, apart_one, apart_in_2, qkv_act, mixed_act, aup, aup_in, asq, asq_in, alog, alog_in,
    stage, acted, right_out, left_out, right_in, left_in, part,
    local_sem, py_s, py_r, px_s, px_r, pd_s, pd_r, pc_s, pc_r, zr_s, zl_s, z_r,
    pz_s, pz_r, na_s, na_r, ap_s, ap_r, c_s, c_r, s1_s, s1_r, s2_s, s2_r, g2_s, g2_r, g1_s, g1_r, gc_s, gc_r,
    sq_s, sq_r, fa_s, fa_r, wo_s, wo_r, wf_s, wf_r, rr_s, rr_r, rl_s, rl_r, au_s, au_r, aq_s, aq_r, al_s, al_r,
):
    n_t, frames, local = sizes
    dp, z, y = lax.axis_index("dp"), lax.axis_index("tensor"), lax.axis_index("section")
    c, x = dp % 2, dp // 2
    me = dp * 2 + y
    place = c * 4 + x * 2 + y
    dp_x, dp_c, y_n = dp + 2 - 4 * x, dp + 1 - 2 * c, 1 - y
    dev_1 = (dp + (1 - c) * (2 - 4 * x), z, y + c * (1 - 2 * y))
    dev_2 = (dp + c * (2 - 4 * x), z, y + (1 - c) * (1 - 2 * y))
    dev_c, dev_x, dev_y = (dp_c, z, y), (dp_x, z, y), (dp, z, y_n)
    b1, b2 = (1 - c) * x + c * y, (1 - c) * y + c * x
    rows = frames * local
    depth, width = wq_hbm.shape
    cols = proj_hbm.shape[1]
    vision = proj_hbm.shape[0]
    chunks = vision // ROWS
    wide = 3 * width
    half, fourth, eighth = wide // 2, wide // 4, wide // 8
    pairs = n_t // 2
    duo = 2 * cols
    heads = width // HD

    def remote(src, dst, send, recv, device):
        return pltpu.make_async_remote_copy(
            src_ref=src, dst_ref=dst, send_sem=send, recv_sem=recv, device_id=device, device_id_type=MESH
        )

    def plane_peer(m):
        g = (me + m) % 8
        return g, (g // 2, z, g % 2)

    own_col = aligned(y * cols, cols)
    loads = [
        pltpu.make_async_copy(proj_hbm, quarter.at[dp, :, pl.ds(own_col, cols)], local_sem.at[0]),
        pltpu.make_async_copy(patches_hbm, patch.at[z], local_sem.at[1]),
        pltpu.make_async_copy(table_hbm, table, local_sem.at[2]),
        pltpu.make_async_copy(wq_hbm, w_ref.at[:, pl.ds(0, width)], local_sem.at[3]),
        pltpu.make_async_copy(wk_hbm, w_ref.at[:, pl.ds(width, width)], local_sem.at[4]),
        pltpu.make_async_copy(wv_hbm, w_ref.at[:, pl.ds(2 * width, width)], local_sem.at[5]),
        pltpu.make_async_copy(wo_hbm, wo_ref.at[me], local_sem.at[6]),
        pltpu.make_async_copy(rows_hbm, rows_ref, local_sem.at[9]),
    ]
    for load in loads:
        load.start()

    barrier = pltpu.get_barrier_semaphore()
    for m in range(1, 8):
        pl.semaphore_signal(barrier, inc=1, device_id=plane_peer(m)[1], device_id_type=MESH)
    for k in range(1, n_t):
        pl.semaphore_signal(barrier, inc=1, device_id=(dp, (z + k) % n_t, y), device_id_type=MESH)
    pl.semaphore_wait(barrier, 7 + n_t - 1)

    def rows_of(i):
        return pl.ds(aligned(i * ROWS, ROWS), ROWS)

    def proj_y(i):
        block = quarter.at[dp, rows_of(i), pl.ds(own_col, cols)]
        return remote(block, block, py_s, py_r.at[i], dev_y)

    def proj_x():
        block = quarter.at[dp, :, pl.ds(own_col, cols)]
        return remote(block, block, px_s, px_r, dev_x)

    def proj_diag():
        at = dp * (1 - c) + dp_x * c
        col = aligned(((1 - c) * (1 - y) + c * y) * cols, cols)
        block = quarter.at[at, :, pl.ds(col, cols)]
        return remote(block, block, pd_s, pd_r, dev_1)

    def proj_core(k):
        block = quarter.at[(dp, dp_x)[k]]
        return remote(block, block, pc_s.at[k], pc_r.at[k], dev_c)

    def patch_send(k, i):
        block = patch.at[z, :, pl.ds(aligned(i * ROWS, ROWS), ROWS)]
        return remote(block, block, pz_s.at[k - 1], pz_r.at[k - 1, i], (dp, (z + k) % n_t, y))

    def act_send(m):
        g, device = plane_peer(m)
        col = aligned(g * depth, depth)
        return remote(nact.at[:, pl.ds(col, depth)], nact_all.at[place], na_s.at[m - 1], na_r.at[m - 1], device)

    def apart_c():
        return remote(apart.at[pl.ds((1 - c) * 4, 4)], apart_in_c, ap_s.at[0], ap_r.at[0], dev_c)

    def apart_1():
        return remote(apart_two.at[pl.ds((1 - b1) * 2, 2)], apart_in_1, ap_s.at[1], ap_r.at[1], dev_1)

    def apart_2():
        return remote(apart_one.at[1 - b2], apart_in_2, ap_s.at[2], ap_r.at[2], dev_2)

    def z_right(p, i, own):
        src = quarter.at[dp, rows_of(i)] if own else pair.at[p, rows_of(i)]
        return remote(src, pair.at[p, rows_of(i)], zr_s.at[p], z_r.at[p, i], (dp, lax.rem(z + 1, n_t), y))

    def z_left(p, i, own):
        src = quarter.at[dp, rows_of(i)] if own else pair.at[p, rows_of(i)]
        return remote(src, pair.at[p, rows_of(i)], zl_s.at[p], z_r.at[p, i], (dp, lax.rem(z + n_t - 1, n_t), y))

    def own_pair(i):
        for p in range(pairs):
            @pl.when(z == pairs * y + p)
            def _():
                @pl.when(z < n_t - 1)
                def _():
                    z_right(p, i, True).start()

                @pl.when(z > 0)
                def _():
                    z_left(p, i, True).start()

                pair[p, rows_of(i)] = quarter[dp, rows_of(i)]

    def spread(i):
        for p in range(pairs):
            home = pairs * y + p

            @pl.when((z > home) & (z < n_t - 1))
            def _():
                z_right(p, i, False).wait_recv()
                z_right(p, i, False).start()

            @pl.when((z < home) & (z > 0))
            def _():
                z_left(p, i, False).wait_recv()
                z_left(p, i, False).start()

    def arrive(i):
        for p in range(pairs):
            home = pairs * y + p

            @pl.when((z != home) & ((z == 0) | (z == n_t - 1)))
            def _():
                z_right(p, i, False).wait_recv()

    loads[0].wait()
    for i in range(chunks):
        proj_y(i).start()
    proj_x().start()
    loads[7].wait()

    slots = frames * SLOTS
    row_at = lax.broadcasted_iota(jnp.int32, (slots, BINS), 0)
    bin_at = lax.broadcasted_iota(jnp.int32, (slots, BINS), 1)

    def one_hot(first):
        index = jnp.full((slots, BINS), -1, jnp.int32)
        for f in range(frames):
            for a in range(ADIM):
                index = jnp.where(row_at == f * SLOTS + first + a, teacher_ref[f, a], index)
        return (index == bin_at).astype(F32)

    def action_stream():
        loads[2].wait()
        looked = jnp.dot(one_hot(1).astype(BF16), table[...], preferred_element_type=F32)
        slot = lax.broadcasted_iota(jnp.int32, looked.shape, 0) % SLOTS
        act[...] = jnp.where(slot == 0, rows_ref[1:2, :].astype(F32), looked)
        rows_f = act[...]
        scale = lax.rsqrt(jnp.mean(rows_f * rows_f, axis=-1, keepdims=True) + eps)
        nact[...] = (rows_f * scale * rows_ref[0:1, :].astype(F32)).astype(BF16)
        nact_all[place] = nact[:, pl.ds(aligned(me * depth, depth), depth)]
        for m in range(1, 8):
            act_send(m).start()

    tile = 512

    def action_partial():
        for m in range(1, 8):
            act_send(m).wait_recv()
        stacked = nact_all[...].reshape(8 * slots, depth)

        def act_tile(j, carry):
            at = pl.ds(aligned(j * tile, tile), tile)
            value = jnp.dot(stacked, w_ref[:, at], preferred_element_type=F32).astype(BF16)
            apart[:, :, at] = value.reshape(8, slots, tile)
            return carry

        lax.fori_loop(0, wide // tile, act_tile, 0)
        apart_c().start()

    def action_sum_1():
        apart_c().wait_recv()
        for one in range(2):
            for two in range(2):
                at = (1 - c) * (2 * one + two) + c * (2 * two + one)
                value = apart[c * 4 + at].astype(F32) + apart_in_c[at].astype(F32)
                apart_two[2 * one + two] = value.astype(BF16)
        apart_1().start()

    def action_sum_2():
        apart_1().wait_recv()
        for two in range(2):
            value = apart_two[2 * b1 + two].astype(F32) + apart_in_1[two].astype(F32)
            apart_one[two] = value.astype(BF16)
        apart_2().start()

    gain_own = rows_ref[0:1, pl.ds(aligned(me * depth, depth), depth)].astype(F32)

    off_c = c * half
    off_1 = off_c + b1 * fourth
    off_2 = off_1 + b2 * eighth

    def at_c(i):
        return remote(send_c.at[i % 2], recv_c.at[i], c_s.at[i % 2], c_r.at[i], dev_c)

    def at_1(i):
        return remote(send_1.at[i % 2], recv_1.at[i], s1_s.at[i % 2], s1_r.at[i], dev_1)

    def at_2(i):
        return remote(send_2.at[i % 2], recv_2.at[i], s2_s.at[i % 2], s2_r.at[i], dev_2)

    def back_2(i):
        block = merged.at[rows_of(i), pl.ds(aligned(off_2), eighth)]
        return remote(block, block, g2_s, g2_r.at[i], dev_2)

    def back_1(i):
        block = merged.at[rows_of(i), pl.ds(aligned(off_1), fourth)]
        return remote(block, block, g1_s, g1_r.at[i], dev_1)

    def back_c(i):
        block = merged.at[rows_of(i), pl.ds(aligned(off_c), half)]
        return remote(block, block, gc_s, gc_r.at[i], dev_c)

    def stage_c(i):
        @pl.when(i >= 2)
        def _():
            at_c(i - 2).wait_send()

        arrive(i)
        block = jnp.concatenate([pair[p, rows_of(i)] for p in range(pairs)], axis=1)
        block = (block.astype(F32) * gain_own).astype(BF16)

        def away(j, carry):
            at = pl.ds(aligned((1 - c) * half + j * tile), tile)
            value = jnp.dot(block, w_ref[:, at], preferred_element_type=F32)
            send_c[i % 2, :, pl.ds(aligned(j * tile, tile), tile)] = value.astype(BF16)
            return carry

        lax.fori_loop(0, half // tile, away, 0)
        at_c(i).start()

        def kept(j, carry):
            at = pl.ds(aligned(c * half + j * tile), tile)
            own_c[i % 2, :, pl.ds(aligned(j * tile, tile), tile)] = jnp.dot(block, w_ref[:, at], preferred_element_type=F32)
            return carry

        lax.fori_loop(0, half // tile, kept, 0)

    def stage_1(i):
        @pl.when(i >= 2)
        def _():
            at_1(i - 2).wait_send()

        at_c(i).wait_recv()
        away = pl.ds(aligned((1 - b1) * fourth), fourth)
        send_1[i % 2] = (own_c[i % 2, :, away] + recv_c[i, :, away].astype(F32)).astype(BF16)
        at_1(i).start()
        kept = pl.ds(aligned(b1 * fourth), fourth)
        own_1[...] = own_c[i % 2, :, kept] + recv_c[i, :, kept].astype(F32)

    def stage_2(i):
        @pl.when(i >= 2)
        def _():
            at_2(i - 2).wait_send()

        at_1(i).wait_recv()
        away = pl.ds(aligned((1 - b2) * eighth), eighth)
        send_2[i % 2] = (own_1[:, away] + recv_1[i, :, away].astype(F32)).astype(BF16)
        at_2(i).start()
        kept = pl.ds(aligned(b2 * eighth), eighth)
        own_2[...] = own_1[:, kept] + recv_1[i, :, kept].astype(F32)

    def stage_3(i):
        at_2(i).wait_recv()
        merged[rows_of(i), pl.ds(aligned(off_2), eighth)] = (own_2[...] + recv_2[i].astype(F32)).astype(BF16)
        back_2(i).start()

    def stage_4(i):
        back_2(i).wait_recv()
        back_1(i).start()

    def stage_5(i):
        back_1(i).wait_recv()
        back_c(i).start()

    def gather_add(first, count):
        for i in range(count):
            back_c(first + i).wait_recv()
        deep = pl.ds(aligned(first * ROWS, ROWS), count * ROWS)
        left = patch[:, :, deep].reshape(n_t * rows, count * ROWS)

        def one(j, carry):
            at = pl.ds(aligned(j * tile, tile), tile)
            value = jnp.dot(left, merged[deep, at], preferred_element_type=F32)

            @pl.when(first == 0)
            def _():
                total[:, at] = value

            @pl.when(first > 0)
            def _():
                total[:, at] += value

            return carry

        lax.fori_loop(0, wide // tile, one, 0)

    def square_send(k):
        to = (z + k) % n_t
        return remote(squares.at[to], squares_in.at[z], sq_s.at[k - 1], sq_r.at[k - 1], (dp, to, y))

    def factor_send(k):
        return remote(factor, factor_in.at[z], fa_s.at[k - 1], fa_r.at[k - 1], (dp, (z + k) % n_t, y))

    def embed():
        for t in range(n_t):
            lanes = jnp.zeros((rows, 128), F32)
            for d in range(quarter.shape[0]):
                value = jnp.dot(patch[t], quarter[d], preferred_element_type=F32).astype(BF16)
                emb[t, :, d * duo : (d + 1) * duo] = value
                value = value.astype(F32)
                value = value * value
                for e in range(duo // 128):
                    lanes = lanes + value[:, e * 128 : (e + 1) * 128]
            squares[t] = lanes
        squares_in[z] = squares[z]
        for k in range(1, n_t):
            square_send(k).start()

    def row_factor():
        for k in range(1, n_t):
            square_send(k).wait_recv()
        lanes = squares_in[0]
        for t in range(1, n_t):
            lanes = lanes + squares_in[t]
        mean = jnp.sum(lanes, axis=-1, keepdims=True) * (1.0 / D)
        factor[...] = jnp.broadcast_to(lax.rsqrt(mean + eps), factor.shape)
        factor_in[z] = factor[...]
        for k in range(1, n_t):
            factor_send(k).start()

    def own_action_rows():
        apart_2().wait_recv()
        qkv_act[...] = (apart_one[b2].astype(F32) + apart_in_2[...].astype(F32)).astype(BF16)

    me_1 = dev_1[0] * 2 + dev_1[2]
    me_2 = dev_2[0] * 2 + dev_2[2]
    me_12 = dp_x * 2 + y_n
    lineage = (me, me_1, me_2, me_12)

    def wo_core(k):
        block = wo_ref.at[lineage[k]]
        return remote(block, block, wo_s.at[k], wo_r.at[k], dev_c)

    pieces = 8
    piece = width // pieces

    def wo_first(i):
        block = wo_ref.at[me, pl.ds(i * piece, piece)]
        return remote(block, block, wf_s, wf_r.at[i], dev_1)

    def wo_second(k):
        block = wo_ref.at[lineage[k]]
        return remote(block, block, wo_s.at[5 + k], wo_r.at[5 + k], dev_2)

    ahead = 3
    proj_y(0).wait_recv()
    own_pair(0)
    proj_y(1).wait_recv()
    own_pair(1)
    action_stream()
    spread(0)
    proj_y(2).wait_recv()
    own_pair(2)
    spread(1)
    for k in (1, 3, 4, 5, 6):
        loads[k].wait()

    def step(s, carry):
        @pl.when(s == 0)
        def _():
            proj_y(ahead).wait_recv()

        @pl.when(s == 1)
        def _():
            for i in range(ahead + 1, chunks):
                proj_y(i).wait_recv()
            proj_x().wait_recv()
            proj_diag().start()
            proj_core(0).start()

        @pl.when(s + ahead < chunks)
        def _():
            own_pair(s + ahead)

        @pl.when((s >= 5) & (s < chunks + 5))
        def _():
            stage_5(s - 5)

        @pl.when((s >= 4) & (s < chunks + 4))
        def _():
            stage_4(s - 4)

        @pl.when((s >= 3) & (s < chunks + 3))
        def _():
            stage_3(s - 3)

        @pl.when((s >= 2) & (s < chunks + 2))
        def _():
            stage_2(s - 2)

        @pl.when((s >= 1) & (s < chunks + 1))
        def _():
            stage_1(s - 1)

        @pl.when(s + 2 < chunks)
        def _():
            spread(s + 2)

        @pl.when(s < chunks)
        def _():
            stage_c(s)

        @pl.when((s >= 1) & (s <= 3))
        def _():
            for k in range(1, n_t):
                patch_send(k, s - 1).start()

        for i in range(3, chunks):
            @pl.when(s == 4 + (i - 3) // 2)
            def _():
                for k in range(1, n_t):
                    patch_send(k, i).start()

        @pl.when((s >= 4) & (s < chunks - 1))
        def _():
            for k in range(1, n_t):
                patch_send(k, s - 4).wait_recv()

        @pl.when(s == chunks - 1)
        def _():
            for i in range(chunks - 5, chunks):
                for k in range(1, n_t):
                    patch_send(k, i).wait_recv()

        @pl.when(s == chunks + 3)
        def _():
            for i in range(3, pieces):
                wo_first(i).start()

        @pl.when((s >= 7) & (s % 2 == 1) & (s < chunks + 3))
        def _():
            gather_add(s - 7, 2)

        @pl.when(s == chunks + 3)
        def _():
            gather_add(chunks - 3, 2)

        @pl.when(s == 0)
        def _():
            action_partial()

        @pl.when(s == 2)
        def _():
            action_sum_1()

        @pl.when(s == 3)
        def _():
            action_sum_2()

        @pl.when(s == 4)
        def _():
            proj_diag().wait_recv()
            proj_core(1).start()
            wo_core(0).start()

        @pl.when(s == chunks - 1)
        def _():
            proj_core(0).wait_recv()
            proj_core(1).wait_recv()
            embed()

        @pl.when(s == chunks + 1)
        def _():
            row_factor()

        for i in range(3):
            @pl.when(s == 1 + i)
            def _():
                wo_first(i).start()

        return carry

    lax.fori_loop(0, chunks + 5, step, 0)
    gather_add(chunks - 1, 1)

    for k in range(1, n_t):
        factor_send(k).wait_recv()

    def scale_tile(j, carry):
        at = pl.ds(aligned(j * tile, tile), tile)
        for t in range(n_t):
            for f in range(frames):
                piece = pl.ds(t * rows + f * local, local)
                value = total[piece, at] * factor_in[t, f * local : (f + 1) * local, 0:1]
                qkv[f, t * local : (t + 1) * local, at] = value.astype(BF16)
        return carry

    lax.fori_loop(0, wide // tile, scale_tile, 0)

    inv_root = 1.0 / math.sqrt(HD)
    length = n_t * local
    nt = (((1,), (1,)), ((), ()))
    block = length // 2
    causal = [
        lax.broadcasted_iota(jnp.int32, (block, (u + 1) * block), 0) + u * block
        >= lax.broadcasted_iota(jnp.int32, (block, (u + 1) * block), 1)
        for u in range(2)
    ]
    slot_i = lax.broadcasted_iota(jnp.int32, (slots, slots), 0)
    slot_j = lax.broadcasted_iota(jnp.int32, (slots, slots), 1)
    slot_sees = (slot_i // SLOTS == slot_j // SLOTS) & (slot_i >= slot_j)
    slot_frame = lax.broadcasted_iota(jnp.int32, (slots, HD), 0) // SLOTS

    def patch_heads(h, carry):
        qc, kc, vc = (pl.ds(aligned(part_at * width + h * HD), HD) for part_at in range(3))
        units = [(f, u) for f in range(frames) for u in range(2)]
        scores = [
            lax.dot_general(
                qkv[f, u * block : (u + 1) * block, qc],
                qkv[f, : (u + 1) * block, kc],
                nt,
                preferred_element_type=F32,
            )
            for f, u in units
        ]
        scores = [jnp.where(causal[u], one * inv_root, -1e30) for one, (f, u) in zip(scores, units)]
        scores = [jnp.exp(one - jnp.max(one, axis=-1, keepdims=True)) for one in scores]
        scores = [(one * (1.0 / jnp.sum(one, axis=-1, keepdims=True))).astype(BF16) for one in scores]
        for one, (f, u) in zip(scores, units):
            value = jnp.dot(one, qkv[f, : (u + 1) * block, vc], preferred_element_type=F32).astype(BF16)
            for t in range(n_t // 2):
                mixed[u * (n_t // 2) + t, f * local : (f + 1) * local, pl.ds(aligned(h * HD), HD)] = value[
                    t * local : (t + 1) * local
                ]
        return carry

    lax.fori_loop(0, heads, patch_heads, 0, unroll=2)

    def action_heads():
        for h in range(heads):
            qc, kc, vc = (pl.ds(part_at * width + h * HD, HD) for part_at in range(3))
            qa, ka, va = qkv_act[:, qc], qkv_act[:, kc], qkv_act[:, vc]
            near = lax.dot_general(qa, ka, nt, preferred_element_type=F32) * inv_root
            near = jnp.where(slot_sees, near, -1e30)
            mixed_slots = jnp.zeros((slots, HD), F32)
            for f in range(frames):
                k, v = qkv[f, :, kc], qkv[f, :, vc]
                far = lax.dot_general(qa, k, nt, preferred_element_type=F32) * inv_root
                top = jnp.maximum(jnp.max(far, axis=-1, keepdims=True), jnp.max(near, axis=-1, keepdims=True))
                far, close = jnp.exp(far - top), jnp.exp(near - top)
                below = 1.0 / (jnp.sum(far, axis=-1, keepdims=True) + jnp.sum(close, axis=-1, keepdims=True))
                value = jnp.dot((far * below).astype(BF16), v, preferred_element_type=F32)
                value = value + jnp.dot((close * below).astype(BF16), va, preferred_element_type=F32)
                mixed_slots = jnp.where(slot_frame == f, value, mixed_slots)
            mixed_act[:, h * HD : (h + 1) * HD] = mixed_slots.astype(BF16)

    def block_of(j, e):
        xs, ys = ((x, y), (x, y), (1 - x, y), (x, 1 - y), (x, 1 - y), (1 - x, y), (1 - x, 1 - y), (1 - x, 1 - y))[
            2 * j + e
        ]
        return 4 * xs + 2 * e + ys

    def contribution(t, j):
        left = mixed[t]
        for e in range(2):
            g = block_of(j, e)
            part[:, e * depth : (e + 1) * depth] = jnp.dot(left, wo_ref[g], preferred_element_type=F32)

            @pl.when(z // pairs == g % 2)
            def _():
                at = pl.ds(aligned(e * depth + (z % pairs) * duo), duo)
                part[:, at] += emb[t, :, pl.ds(aligned((g // 2) * duo), duo)].astype(F32)

    line = n_t - 1

    def to_right(n):
        return remote(right_out.at[n], right_in.at[n], rr_s, rr_r.at[n], (dp, lax.rem(z + 1, n_t), y))

    def to_left(n):
        return remote(left_out.at[n], left_in.at[n], rl_s, rl_r.at[n], (dp, lax.rem(z + n_t - 1, n_t), y))

    def go_right(j, m):
        n = j * line + m
        contribution(line - m, j)

        @pl.when(z > 0)
        def _():
            to_right(n).wait_recv()
            part[...] += right_in[n].astype(F32)

        right_out[n] = part[...].astype(BF16)
        to_right(n).start()

    def go_left(j, m):
        n = j * line + m
        contribution(m, j)

        @pl.when(z < line)
        def _():
            to_left(n).wait_recv()
            part[...] += left_in[n].astype(F32)

        left_out[n] = part[...].astype(BF16)
        to_left(n).start()

    def aup_send(j):
        return remote(aup.at[j], aup_in.at[z], au_s.at[j], au_r.at[z], (dp, j, y))

    def put(j, e):
        at = pl.ds(aligned(block_of(j, e) * depth, depth), depth)
        return pltpu.make_async_copy(stage.at[:, at], out_hbm.at[:, at], local_sem.at[10 + 2 * j + e])

    def finish(j):
        contribution(z, j)

        @pl.when(z > 0)
        def _():
            n = j * line + line - z
            to_right(n).wait_recv()
            part[...] += right_in[n].astype(F32)

        @pl.when(z < n_t - 1)
        def _():
            n = j * line + z
            to_left(n).wait_recv()
            part[...] += left_in[n].astype(F32)

        for e in range(2):
            at = pl.ds(aligned(block_of(j, e) * depth, depth), depth)
            stage[:, at] = part[:, e * depth : (e + 1) * depth].astype(BF16)
            put(j, e).start()

    def asq_send(k):
        return remote(asq, asq_in.at[z], aq_s.at[k - 1], aq_r.at[k - 1], (dp, (z + k) % n_t, y))

    def alog_send(k):
        return remote(alog, alog_in.at[z], al_s.at[k - 1], al_r.at[k - 1], (dp, (z + k) % n_t, y))

    def head_load(j, e):
        at = pl.ds(aligned(block_of(j, e) * depth, depth), depth)
        return pltpu.make_async_copy(head_hbm.at[at], head.at[pl.ds(e * depth, depth)], local_sem.at[7 + e])

    def action_update():
        for j in range(4):
            for e in range(2):
                aup[j, :, e * depth : (e + 1) * depth] = jnp.dot(
                    mixed_act[...], wo_ref[block_of(j, e)], preferred_element_type=F32
                ).astype(BF16)

            @pl.when(z != j)
            def _():
                aup_send(j).start()

            @pl.when(z == j)
            def _():
                for e in range(2):
                    head_load(j, e).start()

    def action_norm():
        for j in range(4):
            @pl.when(z == j)
            def _():
                aup_in[j] = aup[j]
                for t in range(n_t):
                    if t != j:
                        remote(aup.at[j], aup_in.at[t], au_s.at[j], au_r.at[t], (dp, j, y)).wait_recv()
                value = aup_in[0].astype(F32)
                for t in range(1, n_t):
                    value = value + aup_in[t].astype(F32)
                lanes = jnp.zeros((slots, 128), F32)
                for e in range(2):
                    at = pl.ds(aligned(block_of(j, e) * depth, depth), depth)
                    acted_e = value[:, e * depth : (e + 1) * depth] + act[:, at]
                    acted[0, :, e * depth : (e + 1) * depth] = acted_e
                    acted[1, :, e * depth : (e + 1) * depth] = jnp.broadcast_to(
                        rows_ref[2:3, at].astype(F32), (slots, depth)
                    )
                    for q in range(depth // 128):
                        piece = acted_e[:, q * 128 : (q + 1) * 128]
                        lanes = lanes + piece * piece
                asq[...] = lanes

        asq_in[z] = asq[...]
        for k in range(1, n_t):
            asq_send(k).start()

    def action_logits():
        for e in range(2):
            head_load(0, e).wait()
        for k in range(1, n_t):
            asq_send(k).wait_recv()
        lanes = asq_in[0]
        for t in range(1, n_t):
            lanes = lanes + asq_in[t]
        scale = lax.rsqrt(jnp.sum(lanes, axis=-1, keepdims=True) * (1.0 / D) + eps)
        final = (acted[0] * scale * acted[1]).astype(BF16)
        alog[...] = jnp.dot(final, head[...], preferred_element_type=F32)
        alog_in[z] = alog[...]
        for k in range(1, n_t):
            alog_send(k).start()

    def action_loss():
        for k in range(1, n_t):
            alog_send(k).wait_recv()
        logits = alog_in[0]
        for t in range(1, n_t):
            logits = logits + alog_in[t]
        picked = jnp.sum(logits * one_hot(0), axis=-1, keepdims=True)
        top = jnp.max(logits, axis=-1, keepdims=True)
        spread_out = jnp.log(jnp.sum(jnp.exp(logits - top), axis=-1, keepdims=True)) + top
        at_lane = lax.broadcasted_iota(jnp.int32, (slots, 128), 1) == lax.broadcasted_iota(
            jnp.int32, (slots, 128), 0
        ) % SLOTS
        lanes = jnp.where(at_lane, spread_out - picked, 0.0)
        loss_ref[...] = jnp.sum(lanes.reshape(frames, SLOTS, 128), axis=1)[:, :ADIM]

    def drained():
        def left(block, sem):
            remote(block, block, sem, px_r, dev_y).wait_send()

        left(quarter.at[dp, :, pl.ds(own_col, cols)], py_s)
        left(merged.at[:, pl.ds(aligned(off_2), eighth)], g2_s)
        left(merged.at[:, pl.ds(aligned(off_1), fourth)], g1_s)
        left(merged.at[:, pl.ds(aligned(off_c), half)], gc_s)
        for p in range(pairs):
            home = pairs * y + p
            sent = pair.at[p]

            @pl.when((z >= home) & (z < n_t - 1))
            def _():
                left(sent, zr_s.at[p])

            @pl.when((z <= home) & (z > 0))
            def _():
                left(sent, zl_s.at[p])

        for k in range(1, n_t):
            left(patch.at[z], pz_s.at[k - 1])

        for i in range(chunks - 2, chunks):
            at_c(i).wait_send()
            at_1(i).wait_send()
            at_2(i).wait_send()
        for copy in (apart_c(), apart_1(), apart_2()):
            copy.wait_send()
        proj_x().wait_send()
        proj_diag().wait_send()
        for k in range(2):
            proj_core(k).wait_send()
        for m in range(1, 8):
            act_send(m).wait_send()
        for k in range(1, n_t):
            square_send(k).wait_send()
            factor_send(k).wait_send()

    for j in range(4):
        if j == 0:
            wo_core(0).wait_recv()
        elif j == 1:
            own_action_rows()
            action_heads()
            wo_core(1).wait_recv()
        elif j == 2:
            wo_second(0).wait_recv()
            wo_core(2).start()
            wo_second(1).wait_recv()
            wo_core(3).start()
            wo_core(2).wait_recv()
            wo_core(3).wait_recv()
            action_update()
        else:
            action_norm()

        def shift(m, carry):
            t = line - m

            near_right = z < n_t // 2

            @pl.when(near_right & (z < t))
            def _():
                go_right(j, m)

            @pl.when((z >= n_t // 2) & (z > m))
            def _():
                go_left(j, m)

            @pl.when((m >= 1) & (z >= n_t // 2) & (z < t + 1))
            def _():
                go_right(j, m - 1)

            @pl.when((m >= 1) & near_right & (z > m - 1))
            def _():
                go_left(j, m - 1)

            return carry

        shift(0, 0)
        if j == 0:
            for i in range(pieces):
                wo_first(i).wait_recv()
            wo_core(1).start()
            wo_second(0).start()
            wo_second(1).start()
        elif j == 3:
            pl.when((z > 0) & (z < line))(action_logits)
        lax.fori_loop(1, line, shift, 0)
        if j == 3:
            pl.when((z == 0) | (z == line))(action_logits)
        if 0 < j < 3:
            finish(j - 1)
        if j == 1:
            drained()

    finish(2)
    action_loss()
    finish(3)

    for j in range(4):
        for e in range(2):
            put(j, e).wait()
    for k in range(1, n_t):
        asq_send(k).wait_send()
        alog_send(k).wait_send()
    for k in range(4):
        wo_core(k).wait_send()
    remote(wo_ref.at[me], wo_ref.at[me], wf_s, px_r, dev_1).wait_send()
    wo_second(0).wait_send()
    wo_second(1).wait_send()
    for t in range(n_t):
        @pl.when(z == t)
        def _():
            if t < line:
                block = right_out.at[pl.ds(0, 4 * (line - t))]
                remote(block, block, rr_s, px_r, dev_y).wait_send()
            if t > 0:
                block = left_out.at[pl.ds(0, 4 * t)]
                remote(block, block, rl_s, px_r, dev_y).wait_send()

    for j in range(4):
        @pl.when(z != j)
        def _():
            aup_send(j).wait_send()


def fits(mesh, patches, proj_w, wq, wo):
    frames, local, vision = patches.shape
    n_t = mesh.shape["tensor"]
    return (
        mesh.shape["dp"] == 4
        and mesh.shape["section"] == 2
        and n_t == 4
        and proj_w.shape[1] % 128 == 0
        and 8 * wq.shape[0] == D
        and n_t * wq.shape[1] == D
        and vision % ROWS == 0
        and vision // ROWS >= 9
        and vision // ROWS % 2 == 1
        and local % 16 == 0
        and frames * SLOTS % 16 == 0
    )


def program(
    mesh, patches, teacher, proj_w, norm_gain, wq, wk, wv, wo, start_row, action_table, final_gain, head_w
):
    if not fits(mesh, patches, proj_w, wq, wo):
        return on_device(
            patches, teacher, proj_w, norm_gain, wq, wk, wv, wo, start_row, action_table, final_gain, head_w
        )
    frames, local, vision = patches.shape
    n_t = mesh.shape["tensor"]
    rows, slots = frames * local, frames * SLOTS
    depth, width = wq.shape
    cols = proj_w.shape[1]
    wide, chunks, pairs, line = 3 * width, vision // ROWS, n_t // 2, n_t - 1
    row = lax.broadcasted_iota(jnp.int32, (3, D), 0)
    vmem, anywhere = pl.BlockSpec(memory_space=pltpu.VMEM), pl.BlockSpec(memory_space=pl.ANY)
    dma = pltpu.SemaphoreType.DMA
    scratch = [
        pltpu.VMEM((3, D), BF16),
        pltpu.VMEM((depth, wide), BF16),
        pltpu.VMEM((8,) + wo.shape, BF16),
        pltpu.VMEM((4, vision, 2 * cols), BF16),
        pltpu.VMEM((pairs, vision, 2 * cols), BF16),
        pltpu.VMEM((n_t, rows, vision), BF16),
        pltpu.VMEM(action_table.shape, BF16),
        pltpu.VMEM((2 * depth, BINS), BF16),
        pltpu.VMEM((2, ROWS, wide // 2), BF16),
        pltpu.VMEM((chunks, ROWS, wide // 2), BF16),
        pltpu.VMEM((2, ROWS, wide // 4), BF16),
        pltpu.VMEM((chunks, ROWS, wide // 4), BF16),
        pltpu.VMEM((2, ROWS, wide // 8), BF16),
        pltpu.VMEM((chunks, ROWS, wide // 8), BF16),
        pltpu.VMEM((2, ROWS, wide // 2), F32),
        pltpu.VMEM((ROWS, wide // 4), F32),
        pltpu.VMEM((ROWS, wide // 8), F32),
        pltpu.VMEM((vision, wide), BF16),
        pltpu.VMEM((n_t * rows, wide), F32),
        pltpu.VMEM((frames, n_t * local, wide), BF16),
        pltpu.VMEM((n_t, rows, width), BF16),
        pltpu.VMEM((n_t, rows, 8 * cols), BF16),
        pltpu.VMEM((n_t, rows, 128), F32),
        pltpu.VMEM((n_t, rows, 128), F32),
        pltpu.VMEM((rows, 128), F32),
        pltpu.VMEM((n_t, rows, 128), F32),
        pltpu.VMEM((slots, D), F32),
        pltpu.VMEM((slots, D), BF16),
        pltpu.VMEM((8, slots, depth), BF16),
        pltpu.VMEM((8, slots, wide), BF16),
        pltpu.VMEM((4, slots, wide), BF16),
        pltpu.VMEM((4, slots, wide), BF16),
        pltpu.VMEM((2, slots, wide), BF16),
        pltpu.VMEM((2, slots, wide), BF16),
        pltpu.VMEM((slots, wide), BF16),
        pltpu.VMEM((slots, wide), BF16),
        pltpu.VMEM((slots, width), BF16),
        pltpu.VMEM((n_t, slots, 2 * depth), BF16),
        pltpu.VMEM((n_t, slots, 2 * depth), BF16),
        pltpu.VMEM((slots, 128), F32),
        pltpu.VMEM((n_t, slots, 128), F32),
        pltpu.VMEM((slots, BINS), F32),
        pltpu.VMEM((n_t, slots, BINS), F32),
        pltpu.VMEM((rows, D), BF16),
        pltpu.VMEM((2, slots, 2 * depth), F32),
        pltpu.VMEM((4 * line, rows, 2 * depth), BF16),
        pltpu.VMEM((4 * line, rows, 2 * depth), BF16),
        pltpu.VMEM((4 * line, rows, 2 * depth), BF16),
        pltpu.VMEM((4 * line, rows, 2 * depth), BF16),
        pltpu.VMEM((rows, 2 * depth), F32),
        dma((18,)),
        dma, dma((chunks,)),
        dma, dma, dma, dma,
        dma((2,)), dma((2,)),
        dma((pairs,)), dma((pairs,)), dma((pairs, chunks)),
        dma((line,)), dma((line, chunks)),
        dma((7,)), dma((7,)), dma((3,)), dma((3,)),
    ]
    scratch += [dma((2,)), dma((chunks,))] * 3 + [dma, dma((chunks,))] * 3
    scratch += [dma((line,))] * 4
    scratch += [dma((7,))] * 2 + [dma, dma((8,))]
    scratch += [dma, dma((4 * line,))] * 2
    scratch += [dma((n_t,))] * 2 + [dma((line,))] * 4
    hidden, loss = pl.pallas_call(
        functools.partial(fused, (n_t, frames, local)),
        out_shape=(
            jax.ShapeDtypeStruct((rows, D), BF16),
            jax.ShapeDtypeStruct((frames, ADIM), F32),
        ),
        in_specs=[pl.BlockSpec(memory_space=pltpu.SMEM)] + [anywhere] * 9,
        out_specs=(anywhere, vmem),
        scratch_shapes=scratch,
        compiler_params=pltpu.CompilerParams(
            collective_id=0, has_side_effects=True, vmem_limit_bytes=67043328
        ),
    )(
        teacher,
        jnp.where(row == 0, norm_gain[None], jnp.where(row == 1, start_row[None], final_gain[None])),
        patches.reshape(rows, vision),
        proj_w,
        wq,
        wk,
        wv,
        wo,
        action_table,
        head_w,
    )
    return hidden.reshape(frames, local, D), loss


def solution(mesh):
    return jax.shard_map(
        functools.partial(program, mesh),
        mesh=mesh,
        in_specs=(
            P(("dp", "section"), "tensor", None),
            P(("dp", "section"), None),
            P(None, ("dp", "tensor", "section")),
            P(),
            P(("dp", "section"), "tensor"),
            P(("dp", "section"), "tensor"),
            P(("dp", "section"), "tensor"),
            P("tensor", ("dp", "section")),
            P(),
            P(),
            P(),
            P(),
        ),
        out_specs=(P(("dp", "section"), "tensor", None), P(("dp", "section"), None)),
        check_vma=False,
    )
```
